32 devices in a mesh: dp: 16 (over z, y, core), mp: 2 (over x).
Axes of the slice: x: 2, y: 2, z: 4, core: 2. Of those that a mesh axis runs over, the one named last changes fastest.
Arguments:
- tokens: bfloat16 [16384, 1024], P('dp'), may hold values from -6 to 6
- segments: int32 [16384], P('dp'), may hold values from 0 to 1023, as said below
- grad_output: bfloat16 [16384, 1024], P('dp'), may hold values from -6 to 6
- w_qkv: bfloat16 [3, 1024, 1024], P(None, 'dp', 'mp'), may hold values from -0.1875 to 0.1875
- w_out: bfloat16 [1024, 1024], P('mp', 'dp'), may hold values from -0.5 to 0.5
- w_in: bfloat16 [1024, 4096], P('dp', 'mp'), may hold values from -0.1875 to 0.1875
- w_down: bfloat16 [4096, 1024], P('mp', 'dp'), may hold values from -0.09375 to 0.09375
- qv_bias: float32 [2, 16, 64], P(None, 'mp'), may hold values from -1.8 to 1.8
- ffn_bias: float32 [64, 64], P('mp'), may hold values from -3 to 3
- gains: float32 [2, 1024], replicated, may hold values from 0.25 to 1.75
- biases: float32 [4, 1024], replicated, may hold values from -1.8 to 1.8
Outputs:
- activations: bfloat16 [16384, 1024], P('dp')
- grad_tokens: float32 [16384, 1024], P('dp')
- grad_w_qkv: float32 [3, 1024, 1024], P(None, 'dp', 'mp')
- grad_w_out: float32 [1024, 1024], P('mp', 'dp')
- grad_w_in: float32 [1024, 4096], P('dp', 'mp')
- grad_w_down: float32 [4096, 1024], P('mp', 'dp')
- grad_qv_bias: float32 [2, 16, 64], P(None, 'mp', 'dp')
- grad_ffn_bias: float32 [64, 64], P('mp', 'dp')
- grad_gains: float32 [2, 1024], P(None, 'dp')
- grad_biases: float32 [4, 1024], P(None, 'dp')
The draws below stay inside these ranges and needn't reach their ends.
Inputs may be any that keep to these rules, and one draw needn't show every extreme that they name: `segments`: A token's id is the position, among its device's 1024 tokens, of the first token of its sequence, so ids never decrease along a device's tokens; each sequence lies inside one aligned block of 512 tokens, each device's first block is one sequence of exactly 512 tokens, and each device's last token is a sequence of its own.
All inputs are finite; a program needn't handle non-finite values.
Results may differ from the reference program's by a relative error of at most 0.017.
Values may be sent and summed in bfloat16 or wider, within the bound.
A program may use at most 192 MiB of HBM per device.

```python
import jax
import jax.numpy as jnp
from jax import lax

D = 1024
HEADS = 16
HEAD = 64
FF = 4096
TOK_DEV = 1024
BLOCK = 512
TOKENS = 16384
N_MP = 2


def draw_tokens(key, part):
    values_drawn = jax.random.normal(key, (TOKENS, D), jnp.float32)
    return jnp.clip(values_drawn, -6.0, 6.0).astype(jnp.bfloat16)


def draw_segments(key, part):
    per_device = TOKENS // TOK_DEV
    position = jnp.arange(TOKENS, dtype=jnp.int32) % TOK_DEV
    coin_flip = jax.random.randint(key, (TOKENS,), 0, max(BLOCK // 8, 2))
    later = jnp.where(position < BLOCK, 0, (coin_flip == 0).astype(jnp.int32))
    starts = jnp.where(position % BLOCK == 0, 1, later)
    starts = jnp.where(position == TOK_DEV - 1, 1, starts).astype(jnp.int32)
    start_pos = jnp.where(starts == 1, position, 0).astype(jnp.int32)
    segment_ids = lax.cummax(start_pos.reshape(per_device, TOK_DEV), axis=1)
    return segment_ids.reshape(TOKENS).astype(jnp.int32)


def block_levels(own_key, shape, cuts, smallest, top_value):
    level, own = 1.0, jax.random.fold_in(own_key, 6)
    for dim, shards_of in cuts:
        draws = jnp.exp(jax.random.uniform(jax.random.fold_in(own, dim), (shards_of,), jnp.float32, smallest / len(cuts), top_value / len(cuts)))
        level = level * jnp.repeat(draws, shape[dim] // shards_of).reshape([-1 if axis == dim else 1 for axis in range(len(shape))])
    return level


def scatter_about(rng, extent, width, bound, shards=(), kind=jnp.bfloat16):
    level = block_levels(rng, extent, shards, -0.22, 0.18) if shards else 1.0
    entries = jax.random.normal(rng, extent, jnp.float32) * width * level
    return jnp.minimum(jnp.maximum(entries, -bound), bound).astype(kind)


def setup_inputs(seed: int = 0) -> dict:
    splits = jax.random.split(jax.random.key(seed), 12)
    return {
        "tokens": draw_tokens(jax.random.fold_in(splits[11], 71), 0),
        "segments": draw_segments(jax.random.fold_in(splits[11], 71), 0),
        "grad_output": scatter_about(splits[2], (TOKENS, D), 1.0, 6.0, ((0, 16),)),
        "w_qkv": scatter_about(splits[3], (3, D, D), D ** -0.5, 0.1875, ((1, 16), (2, 2))),
        "w_out": scatter_about(splits[4], (D, D), (D // 8) ** -0.5, 0.5, ((0, 2), (1, 16))),
        "w_in": scatter_about(splits[5], (D, FF), D ** -0.5, 0.1875, ((0, 16), (1, 2))),
        "w_down": scatter_about(splits[6], (FF, D), FF ** -0.5, 0.09375, ((0, 2), (1, 16))),
        "qv_bias": scatter_about(splits[7], (2, HEADS, HEAD), 0.3, 1.8, ((1, 2),), jnp.float32),
        "ffn_bias": scatter_about(splits[8], (FF // HEAD, HEAD), 0.5, 3.0, ((0, 2),), jnp.float32),
        "gains": jnp.clip(1.0 + 0.15 * jax.random.normal(splits[9], (2, D), jnp.float32), 0.25, 1.75),
        "biases": scatter_about(splits[10], (4, D), 0.3, 1.8, (), jnp.float32),
    }


EPS = 1e-05
HALF = jnp.bfloat16
FULL = jnp.float32

def rounded(value):
    return value.astype(HALF)

def through_half(value):
    return lax.optimization_barrier(value.astype(HALF)).astype(FULL)

def matmul(left, right):
    return jnp.dot(left, right, preferred_element_type=FULL)

def gelu_grad(pre_act):
    return 0.5 * (1.0 + jax.scipy.special.erf(pre_act * 0.7071067811865476)) + pre_act * jnp.exp(-0.5 * pre_act * pre_act) * 0.3989422804014327

def normalize(summed):
    centered = summed - lax.optimization_barrier(jnp.mean(summed, axis=-1, keepdims=True))
    inv_std = lax.rsqrt(lax.optimization_barrier(jnp.mean(centered * centered, axis=-1, keepdims=True)) + EPS)
    return (centered * inv_std, inv_std)

def norm_back(grad_in, normed, inv_std, gain):
    scaled = grad_in * gain
    return inv_std * (scaled - lax.optimization_barrier(jnp.mean(scaled, axis=-1, keepdims=True)) - normed * lax.optimization_barrier(jnp.mean(scaled * normed, axis=-1, keepdims=True)))

def model_sum(left, right):
    group_width = left.shape[1] // N_MP
    running = jnp.zeros((left.shape[0], right.shape[1]), FULL)
    for member in range(N_MP):
        lower = member * group_width
        partial_term = matmul(left[:, lower:lower + group_width], right[lower:lower + group_width])
        running = running + through_half(partial_term)
    return running

def input_sum(grad_qkv, w_qkv):
    group_width = D // N_MP
    running = jnp.zeros((grad_qkv.shape[1], D), FULL)
    for member in range(N_MP):
        lower = member * group_width
        partial_term = jnp.einsum('sre,sde->rd', grad_qkv[:, :, lower:lower + group_width].astype(FULL), w_qkv[:, :, lower:lower + group_width].astype(FULL))
        running = running + through_half(partial_term)
    return running

def masked_scores(query_blocks, key_blocks, seg_blocks):
    raw_scores = jnp.einsum('nqhe,nkhe->nhqk', query_blocks.astype(FULL), key_blocks.astype(FULL)) * HEAD ** (-0.5)
    same_seg = seg_blocks[:, None, :, None] == seg_blocks[:, None, None, :]
    return jnp.where(same_seg, raw_scores, -1000000000.0)

def encoder_layer(tok_rows, seg_ids, grad_rows_out, w_qkv, w_out, w_in, w_down, bias_rows, hidden_bias, gains, biases):
    row_count = tok_rows.shape[0]
    blocks_count = row_count // BLOCK
    block_shape = (blocks_count, BLOCK, HEADS, HEAD)
    queries = rounded(matmul(tok_rows, w_qkv[0]) + bias_rows[0])
    keys_half = rounded(matmul(tok_rows, w_qkv[1]))
    values_half = rounded(matmul(tok_rows, w_qkv[2]) + bias_rows[1])
    query_blocks = queries.reshape(block_shape)
    key_blocks = keys_half.reshape(block_shape)
    value_blocks = values_half.reshape(block_shape)
    seg_blocks = seg_ids.reshape(blocks_count, BLOCK)
    score = masked_scores(query_blocks, key_blocks, seg_blocks)
    row_top = lax.optimization_barrier(jnp.max(score, axis=-1, keepdims=True))
    log_total = row_top + jnp.log(lax.optimization_barrier(jnp.sum(jnp.exp(score - row_top), axis=-1, keepdims=True)))
    attn_prob = jnp.exp(score - log_total)
    weights_half = rounded(attn_prob)
    context_blocks = rounded(jnp.einsum('nhqk,nkhe->nqhe', weights_half.astype(FULL), value_blocks.astype(FULL)))
    context = context_blocks.reshape(row_count, D)
    summed = tok_rows.astype(FULL) + model_sum(context, w_out) + biases[2]
    normed1, inv_std1 = normalize(summed)
    middle = normed1 * gains[0] + biases[0]
    middle_half = rounded(middle)
    pre_act = matmul(middle_half, w_in) + hidden_bias
    active = rounded(jax.nn.gelu(pre_act, approximate=False))
    second = middle + model_sum(active, w_down) + biases[3]
    normed2, inv_std2 = normalize(second)
    output = rounded(normed2 * gains[1] + biases[1])
    upstream = grad_rows_out.astype(FULL)
    grad_second = norm_back(upstream, normed2, inv_std2, gains[1])
    grad_second_half = rounded(grad_second)
    grad_down = matmul(active.T, grad_second_half)
    grad_pre = matmul(grad_second_half, w_down.T) * gelu_grad(pre_act)
    grad_pre_half = rounded(grad_pre)
    grad_in = matmul(middle_half.T, grad_pre_half)
    grad_middle = grad_second + model_sum(grad_pre_half, w_in.T)
    grad_summed = norm_back(grad_middle, normed1, inv_std1, gains[0])
    grad_summed_half = rounded(grad_summed)
    grad_out_w = matmul(context.T, grad_summed_half)
    grad_context = rounded(matmul(grad_summed_half, w_out.T)).reshape(block_shape)
    grad_values = jnp.einsum('nhqk,nqhe->nkhe', weights_half.astype(FULL), grad_context.astype(FULL))
    grad_prob = jnp.einsum('nqhe,nkhe->nhqk', grad_context.astype(FULL), value_blocks.astype(FULL))
    row_delta = lax.optimization_barrier(jnp.sum(grad_context.astype(FULL) * context_blocks.astype(FULL), axis=-1))
    row_delta = jnp.transpose(row_delta, (0, 2, 1))[..., None]
    grad_score = rounded(attn_prob * (grad_prob - row_delta) * HEAD ** (-0.5))
    grad_queries = jnp.einsum('nhqk,nkhe->nqhe', grad_score.astype(FULL), key_blocks.astype(FULL)).reshape(row_count, D)
    grad_keys = jnp.einsum('nhqk,nqhe->nkhe', grad_score.astype(FULL), query_blocks.astype(FULL)).reshape(row_count, D)
    grad_values = grad_values.reshape(row_count, D)
    grad_qkv = rounded(jnp.stack([grad_queries, grad_keys, grad_values]))
    grad_qkv_w = jnp.stack([matmul(tok_rows.T, grad_qkv[member]) for member in range(3)])
    grad_tokens = grad_summed + input_sum(grad_qkv, w_qkv)
    grad_bias_rows = jnp.stack([lax.optimization_barrier(jnp.sum(grad_queries, axis=0)), lax.optimization_barrier(jnp.sum(grad_values, axis=0))])
    grad_hidden_bias = lax.optimization_barrier(jnp.sum(grad_pre, axis=0))
    grad_gains = jnp.stack([lax.optimization_barrier(jnp.sum(grad_middle * normed1, axis=0)), lax.optimization_barrier(jnp.sum(upstream * normed2, axis=0))])
    grad_biases = jnp.stack([lax.optimization_barrier(jnp.sum(grad_middle, axis=0)), lax.optimization_barrier(jnp.sum(upstream, axis=0)), lax.optimization_barrier(jnp.sum(grad_summed, axis=0)), lax.optimization_barrier(jnp.sum(grad_second, axis=0))])
    grads = (grad_qkv_w, grad_out_w, grad_in, grad_down, grad_bias_rows, grad_hidden_bias, grad_gains, grad_biases)
    return (output, grad_tokens, grads)

def reference(tokens, segments, grad_output, w_qkv, w_out, w_in, w_down, qv_bias, ffn_bias, gains, biases):
    group_count = TOKENS // TOK_DEV
    bias_rows = qv_bias.reshape(2, D)
    hidden_bias = ffn_bias.reshape(FF)

    def scan_step(totals_in, pieces):
        tok_rows, seg_ids, grad_rows_out = pieces
        output, grad_tokens, grads = encoder_layer(tok_rows, seg_ids, grad_rows_out, w_qkv, w_out, w_in, w_down, bias_rows, hidden_bias, gains, biases)
        totals_out = tuple((left + right for left, right in zip(totals_in, grads)))
        return (totals_out, (output, grad_tokens))
    zero_grads = (jnp.zeros((3, D, D), FULL), jnp.zeros((D, D), FULL), jnp.zeros((D, FF), FULL), jnp.zeros((FF, D), FULL), jnp.zeros((2, D), FULL), jnp.zeros((FF,), FULL), jnp.zeros((2, D), FULL), jnp.zeros((4, D), FULL))
    stacked = (tokens.reshape(group_count, TOK_DEV, D), segments.reshape(group_count, TOK_DEV), grad_output.reshape(group_count, TOK_DEV, D))
    totals, (outputs, grad_rows) = lax.scan(scan_step, zero_grads, stacked)
    return (outputs.reshape(TOKENS, D), grad_rows.reshape(TOKENS, D), totals[0], totals[1], totals[2], totals[3], totals[4].reshape(2, HEADS, HEAD), totals[5].reshape(FF // HEAD, HEAD), totals[6], totals[7])
```

```python
import jax
import jax.numpy as jnp
from jax import lax
from jax.sharding import PartitionSpec as P

HEAD = 64
MB = 2
BLOCK = 512
CORES = 2
OUTER = 4

EPS = 1e-05
HALF = jnp.bfloat16
FULL = jnp.float32


def rounded(value):
    return value.astype(HALF)


def matmul(left, right):
    return jnp.dot(left, right, preferred_element_type=FULL)


def matmul_nt(left, right):
    return lax.dot_general(left, right, (((1,), (1,)), ((), ())), preferred_element_type=FULL)


def matmul_tn(left, right):
    return lax.dot_general(left, right, (((0,), (0,)), ((), ())), preferred_element_type=FULL)


def gelu_grad(pre_act):
    return (
        0.5 * (1.0 + jax.scipy.special.erf(pre_act * 0.7071067811865476))
        + pre_act * jnp.exp(-0.5 * pre_act * pre_act) * 0.3989422804014327
    )


def normalize(summed):
    centered = summed - jnp.mean(summed, axis=-1, keepdims=True)
    inv_std = lax.rsqrt(jnp.mean(centered * centered, axis=-1, keepdims=True) + EPS)
    return (centered * inv_std, inv_std)


def norm_back(grad_in, normed, inv_std, gain):
    scaled = grad_in * gain
    return inv_std * (
        scaled
        - jnp.mean(scaled, axis=-1, keepdims=True)
        - normed * jnp.mean(scaled * normed, axis=-1, keepdims=True)
    )


class Ring:
    def __init__(self, n_dp):
        self.n = n_dp
        self.core = CORES
        self.outer = OUTER if n_dp % (OUTER * CORES) == 0 else 1
        self.inner = n_dp // (self.outer * self.core)

    def split(self, index):
        return index // (self.inner * self.core), (index // self.core) % self.inner, index % self.core

    def join(self, outer, inner, core):
        return (outer * self.inner + inner) * self.core + core

    def perm(self, step_outer=0, step_inner=0, step_core=0):
        pairs = []
        for source in range(self.n):
            o, i, c = self.split(source)
            target = self.join(
                (o + step_outer) % self.outer, (i + step_inner) % self.inner, (c + step_core) % self.core
            )
            pairs.append((source, target))
        return pairs

    def send(self, value, **steps):
        return lax.ppermute(value, "dp", self.perm(**steps))

    def order(self, me):
        o, i, c = self.split(me)
        places = []
        for kc in range(self.core):
            for ki in range(self.inner):
                for ko in range(self.outer):
                    places.append(
                        self.join((o - ko) % self.outer, (i - ki) % self.inner, (c - kc) % self.core)
                    )
        return jnp.stack(places)

    def gather(self, shard):
        outer_pieces = [shard]
        for _ in range(self.outer - 1):
            outer_pieces.append(self.send(outer_pieces[-1], step_outer=1))
        columns = [outer_pieces]
        for _ in range(self.inner - 1):
            columns.append([self.send(piece, step_inner=1) for piece in columns[-1]])
        own = [piece for column in columns for piece in column]
        layers = [own]
        for _ in range(self.core - 1):
            layers.append([self.send(piece, step_core=1) for piece in layers[-1]])
        return jnp.concatenate([piece for layer in layers for piece in layer], axis=0)

    def scatter(self, grad):
        rows = grad.shape[0] // self.n
        half = rows * self.inner * self.outer
        grad = rounded(grad)
        running = grad[half : 2 * half]
        running = grad[:half].astype(FULL) + self.send(running, step_core=1).astype(FULL)
        part = rows * self.outer
        pieces = [running[k * part : (k + 1) * part] for k in range(self.inner)]
        total = pieces[1 % self.inner]
        for step in range(1, self.inner):
            arrived = self.send(rounded(total), step_inner=1).astype(FULL)
            total = arrived + pieces[(step + 1) % self.inner]
        blocks = [total[k * rows : (k + 1) * rows] for k in range(self.outer)]
        total = blocks[1 % self.outer]
        for step in range(1, self.outer):
            arrived = self.send(rounded(total), step_outer=1).astype(FULL)
            total = arrived + blocks[(step + 1) % self.outer]
        return total

    def total(self, value):
        for name, count in (("step_core", self.core), ("step_inner", self.inner), ("step_outer", self.outer)):
            if count > 1:
                value = value + sum(self.send(value, **{name: k}) for k in range(1, count))
        return value


def model_sum(term, n_mp):
    term = rounded(term)
    if n_mp == 2:
        other = lax.ppermute(term, "mp", [(0, 1), (1, 0)])
        return term.astype(FULL) + other.astype(FULL)
    return lax.psum(term, "mp").astype(FULL)


def attention_forward(queries, keys, values, segments):
    rows, width = queries.shape
    shape = (rows // BLOCK, BLOCK, width // HEAD, HEAD)
    score = masked_scores(queries.reshape(shape), keys.reshape(shape), segments.reshape(-1, BLOCK))
    row_top = jnp.max(score, axis=-1, keepdims=True)
    log_total = row_top + jnp.log(jnp.sum(jnp.exp(score - row_top), axis=-1, keepdims=True))
    weights = rounded(jnp.exp(score - log_total))
    context = jnp.einsum("nhqk,nkhe->nqhe", weights, values.reshape(shape), preferred_element_type=FULL)
    return rounded(context).reshape(rows, width), log_total


def masked_scores(query_blocks, key_blocks, seg_blocks):
    raw_scores = jnp.einsum(
        "nqhe,nkhe->nhqk", query_blocks, key_blocks, preferred_element_type=FULL
    ) * HEAD ** (-0.5)
    same_seg = seg_blocks[:, None, :, None] == seg_blocks[:, None, None, :]
    return jnp.where(same_seg, raw_scores, -1000000000.0)


def attention_backward(queries, keys, values, segments, log_total, context, grad_context):
    rows, width = queries.shape
    shape = (rows // BLOCK, BLOCK, width // HEAD, HEAD)
    q, k, v, gc = (a.reshape(shape) for a in (queries, keys, values, grad_context))
    score = masked_scores(q, k, segments.reshape(-1, BLOCK))
    attn_prob = jnp.exp(score - log_total)
    weights = rounded(attn_prob)
    grad_values = jnp.einsum("nhqk,nqhe->nkhe", weights, gc, preferred_element_type=FULL)
    grad_prob = jnp.einsum("nqhe,nkhe->nhqk", gc, v, preferred_element_type=FULL)
    row_delta = jnp.sum(gc.astype(FULL) * context.reshape(shape).astype(FULL), axis=-1)
    row_delta = jnp.transpose(row_delta, (0, 2, 1))[..., None]
    grad_score = rounded(attn_prob * (grad_prob - row_delta) * HEAD ** (-0.5))
    grad_queries = jnp.einsum("nhqk,nkhe->nqhe", grad_score, k, preferred_element_type=FULL)
    grad_keys = jnp.einsum("nhqk,nqhe->nkhe", grad_score, q, preferred_element_type=FULL)
    return tuple(g.reshape(rows, width) for g in (grad_queries, grad_keys, grad_values))


def per_device(
    n_dp, n_mp,
    tokens, segments, grad_output, w_qkv, w_out, w_in, w_down, qv_bias, ffn_bias, gains, biases
):
    ring = Ring(n_dp)
    me = lax.axis_index("dp")
    width = w_qkv.shape[2]
    rows, depth = tokens.shape
    piece = depth // n_dp

    qkv_shard = jnp.concatenate([w_qkv[0], w_qkv[1], w_qkv[2]], axis=1)
    g_qkv = ring.gather(qkv_shard)
    g_out = ring.gather(w_out.T)
    g_in = ring.gather(w_in)
    g_down = ring.gather(w_down.T)

    order = ring.order(me)
    column = jnp.repeat(order * piece, piece) + jnp.tile(jnp.arange(piece), n_dp)
    chosen = (jnp.arange(depth)[:, None] == column[None, :]).astype(HALF)
    gains_p = jnp.take(gains.reshape(2, n_dp, piece), order, axis=1).reshape(2, depth)
    biases_p = jnp.take(biases.reshape(4, n_dp, piece), order, axis=1).reshape(4, depth)
    tok_p = rounded(matmul(tokens, chosen))
    up_p = rounded(matmul(grad_output, chosen))

    def unpermute(value):
        return matmul_nt(value, chosen)

    bias_rows = qv_bias.reshape(2, width)
    hidden_bias = ffn_bias.reshape(-1)
    size = rows // MB
    parts = [slice(m * size, (m + 1) * size) for m in range(MB)]
    saved = []
    outputs = []
    for part in parts:
        tok = tok_p[part]
        seg = segments[part]
        projected = matmul(tok, g_qkv)
        queries = rounded(projected[:, :width] + bias_rows[0])
        keys = rounded(projected[:, width : 2 * width])
        values = rounded(projected[:, 2 * width :] + bias_rows[1])
        context, log_total = attention_forward(queries, keys, values, seg)
        attended = model_sum(matmul_nt(context, g_out), n_mp)
        saved.append(dict(tok=tok, seg=seg, q=queries, k=keys, v=values, lse=log_total, ctx=context, att=attended))
    for s in saved:
        summed = s["tok"].astype(FULL) + s["att"] + biases_p[2]
        s["n1"], s["i1"] = normalize(summed)
        s["mid"] = s["n1"] * gains_p[0] + biases_p[0]
        s["midh"] = rounded(s["mid"])
        s["pre"] = matmul(s["midh"], g_in) + hidden_bias
        s["act"] = rounded(jax.nn.gelu(s["pre"], approximate=False))
        s["ffn"] = model_sum(matmul_nt(s["act"], g_down), n_mp)
    for s, part in zip(saved, parts):
        second = s["mid"] + s["ffn"] + biases_p[3]
        s["n2"], s["i2"] = normalize(second)
        outputs.append(rounded(unpermute(rounded(s["n2"] * gains_p[1] + biases_p[1]))))
        s["up"] = up_p[part].astype(FULL)
        s["gs"] = norm_back(s["up"], s["n2"], s["i2"], gains_p[1])
        s["gsh"] = rounded(s["gs"])
        s["gpre"] = matmul(s["gsh"], g_down) * gelu_grad(s["pre"])
        s["gpreh"] = rounded(s["gpre"])
        s["back"] = model_sum(matmul_nt(s["gpreh"], g_in), n_mp)

    def over_tokens(left, right):
        return sum(matmul_tn(s[left], s[right]) for s in saved)

    grad_down = ring.scatter(over_tokens("gsh", "act"))
    grad_in = ring.scatter(over_tokens("midh", "gpreh"))
    for s in saved:
        s["gm"] = s["gs"] + s["back"]
        s["gsum"] = norm_back(s["gm"], s["n1"], s["i1"], gains_p[0])
        s["gsumh"] = rounded(s["gsum"])
        low = rounded(s["gsum"] - s["gsumh"].astype(FULL))
        s["gsum_abs"] = unpermute(s["gsumh"]) + unpermute(low)
        grad_context = rounded(matmul(s["gsumh"], g_out))
        grads = attention_backward(s["q"], s["k"], s["v"], s["seg"], s["lse"], s["ctx"], grad_context)
        s["gq"], s["gv"] = grads[0], grads[2]
        s["gqkv"] = jnp.concatenate([rounded(g) for g in grads], axis=1)
        term = unpermute(rounded(matmul_nt(s["gqkv"], g_qkv)))
        s["gtok"] = s["gsum_abs"] + model_sum(term, n_mp)
    grad_out = ring.scatter(over_tokens("gsumh", "ctx"))
    grad_qkv = ring.scatter(over_tokens("tok", "gqkv"))

    def columns(f):
        return sum(jnp.sum(f(s), axis=0) for s in saved)

    small = ring.total(
        jnp.concatenate(
            [
                absolute(columns(lambda s: s["gm"] * s["n1"]), order, n_dp),
                absolute(columns(lambda s: s["up"] * s["n2"]), order, n_dp),
                absolute(columns(lambda s: s["gm"]), order, n_dp),
                absolute(columns(lambda s: s["up"]), order, n_dp),
                absolute(columns(lambda s: s["gsum"]), order, n_dp),
                absolute(columns(lambda s: s["gs"]), order, n_dp),
                columns(lambda s: s["gq"]),
                columns(lambda s: s["gv"]),
                columns(lambda s: s["gpre"]),
            ]
        )
    )
    norms = lax.dynamic_slice(small[: 6 * depth].reshape(6, depth), (0, me * piece), (6, piece))
    bit = HEAD // n_dp
    rest = small[6 * depth :].reshape(-1, HEAD)
    rest = lax.dynamic_slice(rest, (0, me * bit), (rest.shape[0], bit))
    n_heads = width // HEAD
    return (
        jnp.concatenate(outputs, axis=0),
        jnp.concatenate([s["gtok"] for s in saved], axis=0),
        jnp.stack(jnp.split(grad_qkv, 3, axis=1)),
        grad_out.T,
        grad_in,
        grad_down.T,
        rest[: 2 * n_heads].reshape(2, n_heads, bit),
        rest[2 * n_heads :],
        norms[:2],
        norms[2:],
    )


def absolute(vector, order, n_dp):
    blocks = vector.reshape(n_dp, -1)
    place = jnp.argmax(order[None, :] == jnp.arange(n_dp)[:, None], axis=1)
    return jnp.take(blocks, place, axis=0).reshape(-1)


def solution(mesh):
    n_dp, n_mp = mesh.shape["dp"], mesh.shape["mp"]
    placed = (
        P("dp", None),
        P("dp"),
        P("dp", None),
        P(None, "dp", "mp"),
        P("mp", "dp"),
        P("dp", "mp"),
        P("mp", "dp"),
        P(None, "mp", None),
        P("mp", None),
        P(),
        P(),
    )

    def body(*args):
        return per_device(n_dp, n_mp, *args)

    return jax.shard_map(
        body,
        mesh=mesh,
        in_specs=placed,
        out_specs=(
            P("dp", None),
            P("dp", None),
            P(None, "dp", "mp"),
            P("mp", "dp"),
            P("dp", "mp"),
            P("mp", "dp"),
            P(None, "mp", "dp"),
            P("mp", "dp"),
            P(None, "dp"),
            P(None, "dp"),
        ),
        check_vma=False,
    )
```

```python
import functools

import jax
import jax.numpy as jnp
from jax import lax
from jax.experimental import pallas as pl
from jax.experimental.pallas import tpu as pltpu
from jax.sharding import PartitionSpec as P

HEAD = 64
BLOCK = 512
CORES = 2
OUTER = 4
LANES = 128
CHUNK = 512

EPS = 1e-05
HALF = jnp.bfloat16
FULL = jnp.float32
MESH = pl.DeviceIdType.MESH
VMEM = pl.BlockSpec(memory_space=pltpu.VMEM)
ANY = pl.BlockSpec(memory_space=pl.ANY)
DMA = pltpu.SemaphoreType.DMA


def rounded(value):
    return value.astype(HALF)


def dot(left, right, left_dim=1, right_dim=0):
    return lax.dot_general(
        left, right, (((left_dim,), (right_dim,)), ((), ())), preferred_element_type=FULL
    )


def normalize(summed):
    centered = summed - jnp.mean(summed, axis=-1, keepdims=True)
    inv_std = lax.rsqrt(jnp.mean(centered * centered, axis=-1, keepdims=True) + EPS)
    return (centered * inv_std, inv_std)


def norm_back(grad_in, normed, inv_std, gain):
    scaled = grad_in * gain
    return inv_std * (
        scaled
        - jnp.mean(scaled, axis=-1, keepdims=True)
        - normed * jnp.mean(scaled * normed, axis=-1, keepdims=True)
    )


def column_sum(value):
    return jnp.sum(value, axis=0, keepdims=True)


class Ring:
    def __init__(self, n_dp):
        self.n = n_dp
        self.core = CORES
        self.outer = OUTER if n_dp % (OUTER * CORES) == 0 else 1
        self.inner = n_dp // (self.outer * self.core)

    def split(self, index):
        return index // (self.inner * self.core), (index // self.core) % self.inner, index % self.core

    def join(self, outer, inner, core):
        return (outer * self.inner + inner) * self.core + core


class Place:
    def __init__(self, ring):
        self.ring = ring
        self.z, self.y, self.c = ring.split(lax.axis_index("dp"))
        self.z_next = ring.join((self.z + 1) % ring.outer, self.y, self.c)
        self.z_last = ring.join((self.z + ring.outer - 1) % ring.outer, self.y, self.c)
        self.y_next = ring.join(self.z, (self.y + 1) % ring.inner, self.c)
        self.y_last = ring.join(self.z, (self.y + ring.inner - 1) % ring.inner, self.c)
        self.partner = ring.join(self.z, self.y, 1 - self.c)

    def enter(self, n_mp=1):
        peers = [{"dp": self.partner}]
        if self.ring.outer > 1:
            peers += [{"dp": self.z_next}, {"dp": self.z_last}]
        if self.ring.inner > 1:
            peers += [{"dp": self.y_next}]
        if self.ring.inner > 2:
            peers += [{"dp": self.y_last}]
        x = lax.axis_index("mp")
        peers += [{"mp": (x + k) % n_mp} for k in range(1, n_mp)]
        barrier = pltpu.get_barrier_semaphore()
        for peer in peers:
            pl.semaphore_signal(barrier, inc=1, device_id=peer, device_id_type=MESH)
        pl.semaphore_wait(barrier, len(peers))


def copy_to(source, target, send_sem, recv_sem, device):
    return pltpu.make_async_remote_copy(
        src_ref=source, dst_ref=target, send_sem=send_sem, recv_sem=recv_sem,
        device_id=device, device_id_type=MESH,
    )


class Gather:
    def __init__(self, place, shard, out, sems):
        self.p, self.shard, self.out = place, shard, out
        self.own_sem, self.zs, self.zr, self.ys, self.yr, self.cs, self.cr = sems
        self.rows = shard.shape[0]
        self.sent, self.z_in, self.y_in, self.c_in = [], {}, {}, []
        self.own = pltpu.make_async_copy(shard, self.at(place.z, place.y, place.c), self.own_sem)

    def at(self, z, y, c):
        start = self.p.ring.join(z, y, c) * self.rows
        return self.out.at[pl.ds(pl.multiple_of(start, self.rows), self.rows)]

    def send(self, source, target, send_sem, recv_sem, device):
        copy = copy_to(source, target, send_sem, recv_sem, {"dp": device})
        copy.start()
        self.sent.append(copy)
        return copy

    def along_z(self, k):
        p, ring = self.p, self.p.ring
        target = self.at((p.z + ring.outer - k) % ring.outer, p.y, p.c)
        source = target
        if k == 0:
            self.own.start()
            source = self.shard
        else:
            self.z_in[k].wait_recv()
        if k < ring.outer - 1:
            self.z_in[k + 1] = self.send(source, target, self.zs.at[k], self.zr.at[k], p.z_next)
        if ring.inner > 1:
            self.y_in[k, 1] = self.send(source, target, self.ys.at[k, 0], self.yr.at[k, 0], p.y_next)
        self.c_in.append(self.send(source, target, self.cs.at[k, 0], self.cr.at[k, 0], p.partner))

    def along_y(self, k, step=1):
        p, ring = self.p, self.p.ring
        if step >= ring.inner:
            return
        target = self.at((p.z + ring.outer - k) % ring.outer, (p.y + ring.inner - step) % ring.inner, p.c)
        self.y_in[k, step].wait_recv()
        if step < ring.inner - 1:
            self.y_in[k, step + 1] = self.send(
                target, target, self.ys.at[k, step], self.yr.at[k, step], p.y_next
            )
        self.c_in.append(
            self.send(target, target, self.cs.at[k, step], self.cr.at[k, step], p.partner)
        )

    def rest_y(self, k):
        for step in range(2, self.p.ring.inner):
            self.along_y(k, step)

    def arrived(self):
        for copy in self.c_in:
            copy.wait_recv()
        self.own.wait()

    def finish(self):
        for copy in self.sent:
            copy.wait_send()

    @staticmethod
    def scratch(ring):
        z, y = max(ring.outer - 1, 1), max(ring.inner - 1, 1)
        return [
            DMA, DMA((z,)), DMA((z,)), DMA((ring.outer, y)), DMA((ring.outer, y)),
            DMA((ring.outer, ring.inner)), DMA((ring.outer, ring.inner)),
        ]


def attend_pair(q_ref, k_ref, v_ref, seg_col, seg_row, ctx_ref, lse_ref, block, pair):
    rows = pl.ds(block * BLOCK, BLOCK)
    lanes = pl.ds(pl.multiple_of(pair * LANES, LANES), LANES)
    keys, values = k_ref[rows, lanes], v_ref[rows, lanes]
    queries = q_ref[rows, lanes] * jnp.asarray(HEAD ** (-0.5), HALF)
    lane = lax.broadcasted_iota(jnp.int32, (BLOCK, LANES), 1)
    same = seg_col[rows, :] == seg_row[pl.ds(block, 1), :]
    per_pair = LANES // HEAD
    context = jnp.zeros((BLOCK, LANES), FULL)
    log_totals = lse_ref[rows, :]
    for j in range(per_pair):
        mine = (lane // HEAD) == j
        score = jnp.where(same, dot(jnp.where(mine, queries, jnp.zeros_like(queries)), keys, 1, 1), -1e9)
        top = jnp.max(score, axis=1, keepdims=True)
        exps = jnp.exp(score - top)
        total = jnp.sum(exps, axis=1, keepdims=True)
        weights = rounded(exps * (1.0 / total))
        context = jnp.where(mine, dot(weights, values), context)
        log_totals = jnp.where(lane == per_pair * pair + j, top + jnp.log(total), log_totals)
    lse_ref[rows, :] = log_totals
    ctx_ref[rows, lanes] = rounded(context)


def forward_kernel(ring, n_mp, *refs):
    tok, seg_col, seg_row, bias, s1, s2, s3 = refs[:7]
    g1, g2, g3, q_ref, k_ref, v_ref, ctx, lse, own, recv = refs[7:17]
    sems = refs[17:]
    per = len(Gather.scratch(ring))
    xs, xr = sems[3 * per :]
    place = Place(ring)
    place.enter(n_mp)
    first, second, third = (
        Gather(place, s, g, sems[i * per : (i + 1) * per])
        for i, (s, g) in enumerate(((s1, g1), (s2, g2), (s3, g3)))
    )
    x = lax.axis_index("mp")
    width = q_ref.shape[1]
    blocks = tok.shape[0] // BLOCK
    last = ring.outer
    for k in range(last):
        first.along_z(k)
        if k >= 1:
            first.along_y(k - 1)
    second.along_z(0)
    first.along_y(last - 1)
    for k in range(last):
        first.rest_y(k)
    steps = [functools.partial(second.along_z, k) for k in range(1, last)]
    later = [functools.partial(third.along_z, 0)]
    for k in range(last):
        later.append(functools.partial(second.along_y, k))
        later.append(functools.partial(second.rest_y, k))
        if k + 1 < last:
            later.append(functools.partial(third.along_z, k + 1))
    for k in range(last):
        later.append(functools.partial(third.along_y, k))
        later.append(functools.partial(third.rest_y, k))
    order = []
    while steps or later:
        if steps:
            order.append(steps.pop(0))
        if later:
            order.append(later.pop(0))
    first.arrived()
    lse[...] = jnp.zeros_like(lse)
    crossing = []
    slots = 4 * blocks

    def relay(slot):
        for step in order[len(order) * slot // slots : len(order) * (slot + 1) // slots]:
            step()

    for block in range(blocks):
        rows = pl.ds(block * BLOCK, BLOCK)
        for s, ref in enumerate((q_ref, k_ref, v_ref)):
            projected = dot(tok[rows, :], g1[:, s * width : (s + 1) * width])
            if s != 1:
                projected = projected + bias[s // 2 : s // 2 + 1, :]
            ref[rows, :] = rounded(projected)
        relay(4 * block)

        def pair_step(pair, carry, block=block):
            attend_pair(q_ref, k_ref, v_ref, seg_col, seg_row, ctx, lse, block, pair)
            return carry

        lax.fori_loop(0, width // LANES, pair_step, 0)
        relay(4 * block + 1)
        own[rows, :] = rounded(dot(ctx[rows, :], g1[:, 3 * width :], 1, 1))
        for k in range(1, n_mp):
            copy = copy_to(
                own.at[rows], recv.at[k - 1, rows], xs.at[block, k - 1], xr.at[block, k - 1],
                {"mp": (x + k) % n_mp},
            )
            copy.start()
            crossing.append(copy)
        relay(4 * block + 2)
        relay(4 * block + 3)
    second.arrived()
    third.arrived()
    for copy in crossing:
        copy.wait_recv()
    for gather in (first, second, third):
        gather.finish()
    for copy in crossing:
        copy.wait_send()


def forward(ring, n_mp, tokens, seg_col, seg_row, bias, shards):
    rows, depth = tokens.shape
    width = bias.shape[1]
    blocks = rows // BLOCK
    shape = jax.ShapeDtypeStruct
    gathered = [shape((ring.n * s.shape[0], s.shape[1]), HALF) for s in shards]
    return pl.pallas_call(
        functools.partial(forward_kernel, ring, n_mp),
        name="forward",
        out_shape=gathered
        + [shape((rows, width), HALF)] * 4
        + [shape((rows, LANES), FULL), shape((rows, depth), HALF), shape((n_mp - 1, rows, depth), HALF)],
        in_specs=[VMEM] * 7,
        out_specs=[VMEM, ANY, ANY] + [VMEM] * 7,
        scratch_shapes=Gather.scratch(ring) * 3 + [DMA((blocks, n_mp - 1))] * 2,
        compiler_params=pltpu.CompilerParams(
            collective_id=0, has_side_effects=True, vmem_limit_bytes=48 << 20
        ),
        cost_estimate=pl.CostEstimate(flops=int(2e10), bytes_accessed=int(2e8), transcendentals=0),
    )(tokens, seg_col, seg_row, bias, *shards)


class Scatter:
    def __init__(self, place, grad, out, bufs):
        self.p, self.grad, self.out = place, grad, out
        self.rows = out.shape[0]
        (self.c_in, self.y_out, self.y_in, self.z_out, self.z_in,
         self.cs, self.cr, self.ys, self.yr, self.zs, self.zr) = bufs
        self.sent, self.c_copy, self.y_copy, self.z_copy = [], {}, {}, {}

    def block(self, z, y, c):
        start = self.p.ring.join(z, y, c) * self.rows
        return self.grad.at[pl.ds(pl.multiple_of(start, self.rows), self.rows)]

    def z_of(self, j):
        return (self.p.z + self.p.ring.outer - j) % self.p.ring.outer

    def y_of(self, i):
        return (self.p.y + self.p.ring.inner - i) % self.p.ring.inner

    def send(self, source, target, send_sem, recv_sem, device):
        copy = copy_to(source, target, send_sem, recv_sem, {"dp": device})
        copy.start()
        self.sent.append(copy)
        return copy

    def order(self):
        outer = self.p.ring.outer
        return [j % outer for j in range(1, outer + 1)]

    def to_core(self, i, j):
        p = self.p
        self.c_copy[i, j] = self.send(
            self.block(self.z_of(j), self.y_of(i), 1 - p.c), self.c_in.at[i, j],
            self.cs.at[i, j], self.cr.at[i, j], p.partner,
        )

    def chip_sum(self, i, j):
        self.c_copy[i, j].wait_recv()
        return self.block(self.z_of(j), self.y_of(i), self.p.c)[...].astype(FULL) + self.c_in[i, j].astype(FULL)

    def along_y(self, i, j):
        total = self.chip_sum(i, j)
        if i > 1:
            self.y_copy[i - 1, j].wait_recv()
            total = total + self.y_in[i - 2, j].astype(FULL)
        self.y_out[i - 1, j] = total.astype(self.y_out.dtype)
        self.y_copy[i, j] = self.send(
            self.y_out.at[i - 1, j], self.y_in.at[i - 1, j],
            self.ys.at[i - 1, j], self.yr.at[i - 1, j], self.p.y_next,
        )

    def along_z(self, j):
        ring = self.p.ring
        total = self.chip_sum(0, j)
        if ring.inner > 1:
            self.y_copy[ring.inner - 1, j].wait_recv()
            total = total + self.y_in[ring.inner - 2, j].astype(FULL)
        step = j if j else ring.outer
        if step > 1:
            self.z_copy[step - 1].wait_recv()
            total = total + self.z_in[step - 2].astype(FULL)
        if j == 0:
            self.out[...] = total
        else:
            self.z_out[j - 1] = total.astype(self.z_out.dtype)
            self.z_copy[j] = self.send(
                self.z_out.at[j - 1], self.z_in.at[j - 1], self.zs.at[j - 1], self.zr.at[j - 1],
                self.p.z_next,
            )

    def finish(self):
        for copy in self.sent:
            copy.wait_send()

    @staticmethod
    def scratch(ring, rows, columns, dtype):
        z, y = max(ring.outer - 1, 1), max(ring.inner - 1, 1)

        def buf(*lead):
            return pltpu.VMEM((*lead, rows, columns), dtype)

        return [
            buf(ring.inner, ring.outer), buf(y, ring.outer), buf(y, ring.outer), buf(z), buf(z),
            DMA((ring.inner, ring.outer)), DMA((ring.inner, ring.outer)),
            DMA((y, ring.outer)), DMA((y, ring.outer)), DMA((z,)), DMA((z,)),
        ]


def scatter_kernel(ring, count, *refs):
    grads, outs, rest = refs[:count], refs[count : 2 * count], refs[2 * count :]
    per = len(rest) // count
    place = Place(ring)
    place.enter()
    flows = [
        Scatter(place, g, o, rest[i * per : (i + 1) * per]) for i, (g, o) in enumerate(zip(grads, outs))
    ]
    order = flows[0].order()
    inner = [i % ring.inner for i in range(1, ring.inner + 1)]
    for i in inner:
        for j in order:
            for flow in flows:
                flow.to_core(i, j)
    for i in inner[:-1]:
        for j in order:
            for flow in flows:
                flow.along_y(i, j)
    for j in order:
        for flow in flows:
            flow.along_z(j)
    for flow in flows:
        flow.finish()


def scatter(ring, grads, name, number):
    count = len(grads)
    scratch = []
    for g in grads:
        scratch += Scatter.scratch(ring, g.shape[0] // ring.n, g.shape[1], g.dtype)
    return pl.pallas_call(
        functools.partial(scatter_kernel, ring, count),
        name=name,
        out_shape=[jax.ShapeDtypeStruct((g.shape[0] // ring.n, g.shape[1]), FULL) for g in grads],
        in_specs=[VMEM] * count,
        out_specs=[VMEM] * count,
        scratch_shapes=scratch,
        compiler_params=pltpu.CompilerParams(
            collective_id=number, has_side_effects=True, vmem_limit_bytes=40 << 20
        ),
        cost_estimate=pl.CostEstimate(flops=0, bytes_accessed=int(1.4e8), transcendentals=0),
    )(*grads)


def spread(terms):
    total = terms[0].astype(FULL)
    for term in terms[1:]:
        total = total + term.astype(FULL)
    return total


def ffn_kernel(terms, aliased, *refs):
    tok, parts, (w_in, w_down, bias, gains, biases) = refs[0], refs[1 : 1 + terms], refs[1 + terms : 6 + terms]
    midh, act, n1, inv1, slope, out, total = refs[6 + terms + aliased :]
    step = pl.program_id(0)

    @pl.when(step == 0)
    def _():
        summed = tok[...].astype(FULL) + spread([p[...] for p in parts]) + biases[2:3, :]
        normed, inv = normalize(summed)
        n1[...] = normed
        inv1[...] = jnp.broadcast_to(inv, inv1.shape)
        midh[...] = rounded(normed * gains[0:1, :] + biases[0:1, :])
        total[...] = jnp.zeros_like(total)

    pre = dot(midh[...], w_in[...]) + bias[...]
    phi = 0.5 * (1.0 + lax.erf(pre * 0.7071067811865476))
    active = rounded(pre * phi)
    act[...] = active
    slope[...] = rounded(phi + pre * jnp.exp(-0.5 * pre * pre) * 0.3989422804014327)
    total[...] += dot(active, w_down[...], 1, 1)

    @pl.when(step == pl.num_programs(0) - 1)
    def _():
        out[...] = rounded(total[...])


def ffn(block, tokens, parts, w_in, w_down, hidden_bias, gains, biases, earlier):
    rows, depth = tokens.shape
    hidden = w_in.shape[1]
    chunk = min(CHUNK, hidden)
    shape = jax.ShapeDtypeStruct
    whole = pl.BlockSpec((BLOCK, depth), lambda j: (block, 0))
    local = pl.BlockSpec((BLOCK, depth), lambda j: (0, 0))
    column = pl.BlockSpec((depth, chunk), lambda j: (0, j))
    fixed = lambda a: pl.BlockSpec(a.shape, lambda j: (0, 0))
    part_specs = [whole if p.shape[0] == rows else local for p in parts]
    n_in = 6 + len(parts)
    return pl.pallas_call(
        functools.partial(ffn_kernel, len(parts), len(earlier)),
        name=f"ffn_{block}",
        grid=(hidden // chunk,),
        out_shape=[
            shape((rows, depth), HALF), shape((rows, hidden), HALF), shape((BLOCK, depth), FULL),
            shape((BLOCK, LANES), FULL), shape((BLOCK, hidden), HALF), shape((BLOCK, depth), HALF),
        ],
        in_specs=[whole] + part_specs
        + [column, column, pl.BlockSpec((1, chunk), lambda j: (0, j)), fixed(gains), fixed(biases)]
        + [ANY] * len(earlier),
        out_specs=[
            whole, pl.BlockSpec((BLOCK, chunk), lambda j: (block, j)), local,
            pl.BlockSpec((BLOCK, LANES), lambda j: (0, 0)), pl.BlockSpec((BLOCK, chunk), lambda j: (0, j)), local,
        ],
        scratch_shapes=[pltpu.VMEM((BLOCK, depth), FULL)],
        input_output_aliases={n_in + i: i for i in range(len(earlier))},
        compiler_params=pltpu.CompilerParams(vmem_limit_bytes=40 << 20),
        cost_estimate=pl.CostEstimate(
            flops=4 * BLOCK * depth * hidden, bytes_accessed=20 << 20, transcendentals=2 * BLOCK * hidden
        ),
    )(tokens, *parts, w_in, w_down, hidden_bias, gains, biases, *earlier)


def ffn_back_kernel(terms, aliased, *refs):
    n1, up, parts = refs[0], refs[1], refs[2 : 2 + terms]
    slope, w_in, w_down, gains, biases = refs[2 + terms : 7 + terms]
    output, gsh, gpreh, gs, sums, pre_sums, out, total = refs[7 + terms + aliased :]
    step = pl.program_id(0)

    @pl.when(step == 0)
    def _():
        middle = n1[...] * gains[0:1, :] + biases[0:1, :]
        second = middle + spread([p[...] for p in parts]) + biases[3:4, :]
        normed, inv = normalize(second)
        output[...] = rounded(normed * gains[1:2, :] + biases[1:2, :])
        upstream = up[...].astype(FULL)
        grad = norm_back(upstream, normed, inv, gains[1:2, :])
        gs[...] = grad
        gsh[...] = rounded(grad)
        sums[...] = jnp.zeros_like(sums)
        sums[0:1, :] = column_sum(upstream * normed)
        sums[1:2, :] = column_sum(upstream)
        sums[2:3, :] = column_sum(grad)
        total[...] = jnp.zeros_like(total)

    grad_pre = dot(gsh[...], w_down[...]) * slope[...].astype(FULL)
    pre_sums[...] = jnp.broadcast_to(column_sum(grad_pre), pre_sums.shape)
    half = rounded(grad_pre)
    gpreh[...] = half
    total[...] += dot(half, w_in[...], 1, 1)

    @pl.when(step == pl.num_programs(0) - 1)
    def _():
        out[...] = rounded(total[...])


def ffn_back(block, n1, grad_output, parts, slope, w_in, w_down, gains, biases, earlier):
    rows, depth = grad_output.shape
    hidden = w_in.shape[1]
    chunk = min(CHUNK, hidden)
    shape = jax.ShapeDtypeStruct
    whole = pl.BlockSpec((BLOCK, depth), lambda j: (block, 0))
    local = pl.BlockSpec((BLOCK, depth), lambda j: (0, 0))
    column = pl.BlockSpec((depth, chunk), lambda j: (0, j))
    fixed = lambda a: pl.BlockSpec(a.shape, lambda j: (0, 0))
    n_in = 7 + len(parts)
    return pl.pallas_call(
        functools.partial(ffn_back_kernel, len(parts), len(earlier)),
        name=f"ffn_back_{block}",
        grid=(hidden // chunk,),
        out_shape=[
            shape((rows, depth), HALF), shape((rows, depth), HALF), shape((rows, hidden), HALF),
            shape((BLOCK, depth), FULL), shape((8, depth), FULL), shape((8, hidden), FULL),
            shape((BLOCK, depth), HALF),
        ],
        in_specs=[local, whole] + [local] * len(parts)
        + [pl.BlockSpec((BLOCK, chunk), lambda j: (0, j)), column, column, fixed(gains), fixed(biases)]
        + [ANY] * len(earlier),
        out_specs=[
            whole, whole, pl.BlockSpec((BLOCK, chunk), lambda j: (block, j)), local,
            pl.BlockSpec((8, depth), lambda j: (0, 0)), pl.BlockSpec((8, chunk), lambda j: (0, j)), local,
        ],
        scratch_shapes=[pltpu.VMEM((BLOCK, depth), FULL)],
        input_output_aliases={n_in + i: i for i in range(len(earlier))},
        compiler_params=pltpu.CompilerParams(vmem_limit_bytes=40 << 20),
        cost_estimate=pl.CostEstimate(
            flops=4 * BLOCK * depth * hidden, bytes_accessed=22 << 20, transcendentals=0
        ),
    )(n1, grad_output, *parts, slope, w_in, w_down, gains, biases, *earlier)


def attend_back_pair(q_ref, k_ref, v_ref, seg_col, seg_row, ctx, lse, gctx, dq, dk, dv, pair):
    lanes = pl.ds(pl.multiple_of(pair * LANES, LANES), LANES)
    keys, values, q = k_ref[:, lanes], v_ref[:, lanes], q_ref[:, lanes]
    queries = q * jnp.asarray(HEAD ** (-0.5), HALF)
    grad = gctx[:, lanes]
    product = grad.astype(FULL) * ctx[:, lanes].astype(FULL)
    lane = lax.broadcasted_iota(jnp.int32, (BLOCK, LANES), 1)
    same = seg_col[...] == seg_row[...]
    per_pair = LANES // HEAD
    log_totals = lse[...]
    grad_q = grad_k = grad_v = jnp.zeros((BLOCK, LANES), FULL)
    for j in range(per_pair):
        mine = (lane // HEAD) == j
        zero = jnp.zeros_like(grad)
        score = jnp.where(same, dot(jnp.where(mine, queries, zero), keys, 1, 1), -1e9)
        log_total = jnp.sum(jnp.where(lane == per_pair * pair + j, log_totals, 0.0), axis=1, keepdims=True)
        delta = jnp.sum(jnp.where(mine, product, 0.0), axis=1, keepdims=True)
        prob = jnp.exp(score - log_total)
        grad_prob = dot(jnp.where(mine, grad, zero), values, 1, 1)
        grad_score = rounded(prob * (grad_prob - delta) * HEAD ** (-0.5))
        grad_q = jnp.where(mine, dot(grad_score, keys), grad_q)
        grad_k = jnp.where(mine, dot(grad_score, q, 0, 0), grad_k)
        grad_v = jnp.where(mine, dot(rounded(prob), grad, 0, 0), grad_v)
    dq[:, lanes], dk[:, lanes], dv[:, lanes] = grad_q, grad_k, grad_v


def attention_back_kernel(terms, aliased, *refs):
    gs, n1, inv1, parts = refs[0], refs[1], refs[2], refs[3 : 3 + terms]
    w1, q_ref, k_ref, v_ref, ctx, lse, seg_col, seg_row, gains = refs[3 + terms : 12 + terms]
    gsumh, dqkv, gsum, sums, head_sums, out, gctx, dq, dk, dv = refs[12 + terms + aliased :]
    width = q_ref.shape[1]
    normed = n1[...]
    grad_middle = gs[...] + spread([p[...] for p in parts])
    grad = norm_back(grad_middle, normed, inv1[:, 0:1], gains[0:1, :])
    gsum[...] = grad
    gsumh[...] = rounded(grad)
    sums[...] = jnp.zeros_like(sums)
    sums[0:1, :] = column_sum(grad_middle * normed)
    sums[1:2, :] = column_sum(grad_middle)
    sums[2:3, :] = column_sum(grad)
    gctx[...] = rounded(dot(gsumh[...], w1[:, 3 * width :]))

    def pair_step(pair, carry):
        attend_back_pair(q_ref, k_ref, v_ref, seg_col, seg_row, ctx, lse, gctx, dq, dk, dv, pair)
        return carry

    lax.fori_loop(0, width // LANES, pair_step, 0)
    head_sums[...] = jnp.zeros_like(head_sums)
    head_sums[0:1, :] = column_sum(dq[...])
    head_sums[1:2, :] = column_sum(dv[...])
    total = None
    for s, part in enumerate((dq, dk, dv)):
        half = rounded(part[...])
        dqkv[:, s * width : (s + 1) * width] = half
        term = dot(half, w1[:, s * width : (s + 1) * width], 1, 1)
        total = term if total is None else total + term
    out[...] = rounded(total)


def attention_back(block, gs, n1, inv1, parts, w1, q, k, v, ctx, lse, seg_col, seg_row, gains, earlier):
    rows, width = q.shape
    depth = gs.shape[1]
    shape = jax.ShapeDtypeStruct
    own = lambda a: pl.BlockSpec((BLOCK, a.shape[1]), lambda i: (block, 0))
    fixed = lambda a: pl.BlockSpec(a.shape, lambda i: (0, 0))
    tile = lambda r, c, b=0: pl.BlockSpec((r, c), lambda i: (b, 0))
    n_in = 12 + len(parts)
    return pl.pallas_call(
        functools.partial(attention_back_kernel, len(parts), len(earlier)),
        name=f"attention_back_{block}",
        grid=(1,),
        out_shape=[
            shape((rows, depth), HALF), shape((rows, 3 * width), HALF), shape((BLOCK, depth), FULL),
            shape((8, depth), FULL), shape((8, width), FULL), shape((BLOCK, depth), HALF),
        ],
        in_specs=[fixed(gs), fixed(n1), fixed(inv1)] + [fixed(p) for p in parts]
        + [fixed(w1), own(q), own(k), own(v), own(ctx), own(lse), own(seg_col),
           pl.BlockSpec((None, 1, BLOCK), lambda i: (block, 0, 0)), fixed(gains)]
        + [ANY] * len(earlier),
        out_specs=[
            tile(BLOCK, depth, block), tile(BLOCK, 3 * width, block), tile(BLOCK, depth),
            tile(8, depth), tile(8, width), tile(BLOCK, depth),
        ],
        scratch_shapes=[pltpu.VMEM((BLOCK, width), HALF)] + [pltpu.VMEM((BLOCK, width), FULL)] * 3,
        input_output_aliases={n_in + i: i for i in range(len(earlier))},
        compiler_params=pltpu.CompilerParams(vmem_limit_bytes=48 << 20),
        cost_estimate=pl.CostEstimate(
            flops=8 * BLOCK * depth * width + 20 * BLOCK * BLOCK * width * 2,
            bytes_accessed=20 << 20, transcendentals=BLOCK * BLOCK * width // HEAD,
        ),
    )(gs, n1, inv1, *parts, w1, q, k, v, ctx, lse, seg_col, seg_row.reshape(-1, 1, BLOCK), gains, *earlier)


def across(term, n_mp):
    shifts = [[(i, (i + k) % n_mp) for i in range(n_mp)] for k in range(1, n_mp)]
    return [term] + [lax.ppermute(term, "mp", shift) for shift in shifts]


def per_device(
    n_dp, n_mp,
    tokens, segments, grad_output, w_qkv, w_out, w_in, w_down, qv_bias, ffn_bias, gains, biases
):
    ring = Ring(n_dp)
    width = w_qkv.shape[2]
    rows, depth = tokens.shape
    piece = depth // n_dp
    n_heads = width // HEAD
    blocks = range(rows // BLOCK)

    shards = [jnp.concatenate([w_qkv[0], w_qkv[1], w_qkv[2], w_out.T], axis=1), w_in, w_down.T]
    seg_col = segments.reshape(rows, 1)
    seg_row = segments.reshape(-1, BLOCK)
    w1, w2, w3, q, k, v, ctx, lse, own, recv = forward(
        ring, n_mp, tokens, seg_col, seg_row, qv_bias.reshape(2, width), shards
    )
    attended = [own] + [recv[i] for i in range(n_mp - 1)]
    hidden_bias = ffn_bias.reshape(1, -1)

    saved, earlier = [], []
    for block in blocks:
        midh, act, n1, inv1, slope, term = ffn(
            block, tokens, attended, w2, w3, hidden_bias, gains, biases, earlier
        )
        earlier = [midh, act]
        saved.append(dict(n1=n1, inv1=inv1, slope=slope, ffn=across(term, n_mp)))
    earlier = []
    for block, s in zip(blocks, saved):
        output, gsh, gpreh, s["gs"], s["sums2"], s["pre"], term = ffn_back(
            block, s["n1"], grad_output, s["ffn"], s["slope"], w2, w3, gains, biases, earlier
        )
        earlier = [output, gsh, gpreh]
        s["back"] = across(term, n_mp)
    grad_down = rounded(dot(gsh, act, 0, 0))
    grad_in = rounded(dot(midh, gpreh, 0, 0))
    grad_down, grad_in = scatter(ring, [grad_down, grad_in], "scatter_ffn", 1)

    earlier, totals = [], []
    for block, s in zip(blocks, saved):
        gsumh, dqkv, gsum, s["sums1"], s["heads"], term = attention_back(
            block, s["gs"], s["n1"], s["inv1"], s["back"], w1, q, k, v, ctx, lse, seg_col, seg_row, gains,
            earlier,
        )
        earlier = [gsumh, dqkv]
        totals.append(gsum + spread(across(term, n_mp)))

    def over(name):
        return sum(s[name] for s in saved)

    sums1, sums2, heads, pre = over("sums1"), over("sums2"), over("heads"), over("pre")
    order = [sums1[0], sums2[0], sums1[1], sums2[1], sums1[2], sums2[2]]
    bit = HEAD // n_dp
    small = jnp.concatenate(
        [
            jnp.stack(order).reshape(6, n_dp, piece).transpose(1, 0, 2).reshape(n_dp, -1),
            heads[:2].reshape(-1, n_dp, bit).transpose(1, 0, 2).reshape(n_dp, -1),
            pre[0].reshape(-1, n_dp, bit).transpose(1, 0, 2).reshape(n_dp, -1),
        ],
        axis=1,
    )
    used = small.shape[1]
    small = jnp.pad(small, ((0, 0), (0, -used % (8 * LANES)))).reshape(-1, LANES)
    grad_qkv = rounded(dot(tokens, dqkv, 0, 0))
    grad_out = rounded(dot(gsumh, ctx, 0, 0))
    grad_qkv, grad_out, small = scatter(ring, [grad_qkv, grad_out, small], "scatter_attention", 2)
    small = small.reshape(-1)
    norms = small[: 6 * piece].reshape(6, piece)
    middle = 6 * piece + 2 * n_heads * bit
    return (
        output,
        jnp.concatenate(totals, axis=0),
        jnp.stack(jnp.split(grad_qkv, 3, axis=1)),
        grad_out.T,
        grad_in,
        grad_down.T,
        small[6 * piece : middle].reshape(2, n_heads, bit),
        small[middle:used].reshape(-1, bit),
        norms[:2],
        norms[2:],
    )


def solution(mesh):
    n_dp, n_mp = mesh.shape["dp"], mesh.shape["mp"]
    placed = (
        P("dp", None),
        P("dp"),
        P("dp", None),
        P(None, "dp", "mp"),
        P("mp", "dp"),
        P("dp", "mp"),
        P("mp", "dp"),
        P(None, "mp", None),
        P("mp", None),
        P(),
        P(),
    )

    def body(*args):
        return per_device(n_dp, n_mp, *args)

    return jax.shard_map(
        body,
        mesh=mesh,
        in_specs=placed,
        out_specs=(
            P("dp", None),
            P("dp", None),
            P(None, "dp", "mp"),
            P("mp", "dp"),
            P("dp", "mp"),
            P("mp", "dp"),
            P(None, "mp", "dp"),
            P("mp", "dp"),
            P(None, "dp"),
            P(None, "dp"),
        ),
        check_vma=False,
    )
```

```python
import functools

import jax
import jax.numpy as jnp
from jax import lax
from jax.experimental import pallas as pl
from jax.experimental.pallas import tpu as pltpu
from jax.sharding import PartitionSpec as P

HEAD = 64
BLOCK = 512
CORES = 2
OUTER = 4
LANES = 128
CHUNK = 512

EPS = 1e-05
HALF = jnp.bfloat16
FULL = jnp.float32
MESH = pl.DeviceIdType.MESH
VMEM = pl.BlockSpec(memory_space=pltpu.VMEM)
ANY = pl.BlockSpec(memory_space=pl.ANY)
DMA = pltpu.SemaphoreType.DMA


def rounded(value):
    return value.astype(HALF)


def dot(left, right, left_dim=1, right_dim=0):
    return lax.dot_general(
        left, right, (((left_dim,), (right_dim,)), ((), ())), preferred_element_type=FULL
    )


def normalize(summed):
    centered = summed - jnp.mean(summed, axis=-1, keepdims=True)
    inv_std = lax.rsqrt(jnp.mean(centered * centered, axis=-1, keepdims=True) + EPS)
    return (centered * inv_std, inv_std)


def norm_back(grad_in, normed, inv_std, gain):
    scaled = grad_in * gain
    return inv_std * (
        scaled
        - jnp.mean(scaled, axis=-1, keepdims=True)
        - normed * jnp.mean(scaled * normed, axis=-1, keepdims=True)
    )


def column_sum(value):
    return jnp.sum(value, axis=0, keepdims=True)


class Ring:
    def __init__(self, n_dp):
        self.n = n_dp
        self.core = CORES
        self.outer = OUTER if n_dp % (OUTER * CORES) == 0 else 1
        self.inner = n_dp // (self.outer * self.core)

    def split(self, index):
        return index // (self.inner * self.core), (index // self.core) % self.inner, index % self.core

    def join(self, outer, inner, core):
        return (outer * self.inner + inner) * self.core + core


class Place:
    def __init__(self, ring):
        self.ring = ring
        self.z, self.y, self.c = ring.split(lax.axis_index("dp"))
        self.z_next = ring.join((self.z + 1) % ring.outer, self.y, self.c)
        self.z_last = ring.join((self.z + ring.outer - 1) % ring.outer, self.y, self.c)
        self.y_next = ring.join(self.z, (self.y + 1) % ring.inner, self.c)
        self.y_last = ring.join(self.z, (self.y + ring.inner - 1) % ring.inner, self.c)
        self.partner = ring.join(self.z, self.y, 1 - self.c)

    def at_z(self, k):
        return self.ring.join((self.z + k) % self.ring.outer, self.y, self.c)

    def at_y(self, k):
        return self.ring.join(self.z, (self.y + k) % self.ring.inner, self.c)

    def enter(self, n_mp=1):
        peers = [{"dp": self.partner}]
        peers += [{"dp": self.at_z(k)} for k in range(1, self.ring.outer)]
        peers += [{"dp": self.at_y(k)} for k in range(1, self.ring.inner)]
        x = lax.axis_index("mp")
        peers += [{"mp": (x + k) % n_mp} for k in range(1, n_mp)]
        barrier = pltpu.get_barrier_semaphore()
        for peer in peers:
            pl.semaphore_signal(barrier, inc=1, device_id=peer, device_id_type=MESH)
        pl.semaphore_wait(barrier, len(peers))


def copy_to(source, target, send_sem, recv_sem, device):
    return pltpu.make_async_remote_copy(
        src_ref=source, dst_ref=target, send_sem=send_sem, recv_sem=recv_sem,
        device_id=device, device_id_type=MESH,
    )


class Gather:
    def __init__(self, place, shard, out, sems):
        self.p, self.shard, self.out = place, shard, out
        self.own_sem, self.zs, self.zr, self.ys, self.yr, self.cs, self.cr = sems
        self.rows = shard.shape[0]
        self.sent, self.z_in, self.y_in, self.c_in = [], {}, {}, []
        self.own = pltpu.make_async_copy(shard, self.at(place.z, place.y, place.c), self.own_sem)

    def at(self, z, y, c):
        start = self.p.ring.join(z, y, c) * self.rows
        return self.out.at[pl.ds(pl.multiple_of(start, self.rows), self.rows)]

    def send(self, source, target, send_sem, recv_sem, device):
        copy = copy_to(source, target, send_sem, recv_sem, {"dp": device})
        copy.start()
        self.sent.append(copy)
        return copy

    def along_z(self, k):
        p, ring = self.p, self.p.ring
        target = self.at((p.z + ring.outer - k) % ring.outer, p.y, p.c)
        source = target
        if k == 0:
            self.own.start()
            source = self.shard
        else:
            self.z_in[k].wait_recv()
        if k < ring.outer - 1:
            self.z_in[k + 1] = self.send(source, target, self.zs.at[k], self.zr.at[k], p.z_next)
        if ring.inner > 1:
            self.y_in[k, 1] = self.send(source, target, self.ys.at[k, 0], self.yr.at[k, 0], p.y_next)
        self.c_in.append(self.send(source, target, self.cs.at[k, 0], self.cr.at[k, 0], p.partner))

    def along_y(self, k, step=1):
        p, ring = self.p, self.p.ring
        if step >= ring.inner:
            return
        target = self.at((p.z + ring.outer - k) % ring.outer, (p.y + ring.inner - step) % ring.inner, p.c)
        self.y_in[k, step].wait_recv()
        if step < ring.inner - 1:
            self.y_in[k, step + 1] = self.send(
                target, target, self.ys.at[k, step], self.yr.at[k, step], p.y_next
            )
        self.c_in.append(
            self.send(target, target, self.cs.at[k, step], self.cr.at[k, step], p.partner)
        )

    def rest_y(self, k):
        for step in range(2, self.p.ring.inner):
            self.along_y(k, step)

    def arrived(self):
        for copy in self.c_in:
            copy.wait_recv()
        self.own.wait()

    def finish(self):
        for copy in self.sent:
            copy.wait_send()

    @staticmethod
    def scratch(ring):
        z, y = max(ring.outer - 1, 1), max(ring.inner - 1, 1)
        return [
            DMA, DMA((z,)), DMA((z,)), DMA((ring.outer, y)), DMA((ring.outer, y)),
            DMA((ring.outer, ring.inner)), DMA((ring.outer, ring.inner)),
        ]


def attend_pair(q_ref, k_ref, v_ref, seg_col, seg_row, ctx_ref, lse_ref, block, pair):
    rows = pl.ds(block * BLOCK, BLOCK)
    lanes = pl.ds(pl.multiple_of(pair * LANES, LANES), LANES)
    keys, values = k_ref[rows, lanes], v_ref[rows, lanes]
    queries = q_ref[rows, lanes] * jnp.asarray(HEAD ** (-0.5), HALF)
    lane = lax.broadcasted_iota(jnp.int32, (BLOCK, LANES), 1)
    same = seg_col[rows, :] == seg_row[pl.ds(block, 1), :]
    per_pair = LANES // HEAD
    context = jnp.zeros((BLOCK, LANES), FULL)
    log_totals = lse_ref[rows, :]
    for j in range(per_pair):
        mine = (lane // HEAD) == j
        score = jnp.where(same, dot(jnp.where(mine, queries, jnp.zeros_like(queries)), keys, 1, 1), -1e9)
        top = jnp.max(score, axis=1, keepdims=True)
        exps = jnp.exp(score - top)
        total = jnp.sum(exps, axis=1, keepdims=True)
        weights = rounded(exps * (1.0 / total))
        context = jnp.where(mine, dot(weights, values), context)
        log_totals = jnp.where(lane == per_pair * pair + j, top + jnp.log(total), log_totals)
    lse_ref[rows, :] = log_totals
    ctx_ref[rows, lanes] = rounded(context)


def forward_kernel(ring, n_mp, *refs):
    tok, seg_col, seg_row, bias, s1, s2, s3 = refs[:7]
    g1, g2, g3, q_ref, k_ref, v_ref, ctx, lse, own, recv = refs[7:17]
    sems = refs[17:]
    per = len(Gather.scratch(ring))
    xs, xr = sems[3 * per :]
    place = Place(ring)
    place.enter(n_mp)
    first, second, third = (
        Gather(place, s, g, sems[i * per : (i + 1) * per])
        for i, (s, g) in enumerate(((s1, g1), (s2, g2), (s3, g3)))
    )
    x = lax.axis_index("mp")
    width = q_ref.shape[1]
    blocks = tok.shape[0] // BLOCK
    last = ring.outer
    for k in range(last):
        first.along_z(k)
        if k >= 1:
            first.along_y(k - 1)
    second.along_z(0)
    first.along_y(last - 1)
    for k in range(last):
        first.rest_y(k)
    z2 = [functools.partial(second.along_z, k) for k in range(1, last)]
    z3 = [functools.partial(third.along_z, k) for k in range(last)]
    first.arrived()
    lse[...] = jnp.zeros_like(lse)
    crossing = []

    def relay(steps, count=1):
        for _ in range(min(count, len(steps))):
            steps.pop(0)()

    relay(z2)
    for block in range(blocks):
        rows = pl.ds(block * BLOCK, BLOCK)
        for s, ref in enumerate((q_ref, k_ref, v_ref)):
            projected = dot(tok[rows, :], g1[:, s * width : (s + 1) * width])
            if s != 1:
                projected = projected + bias[s // 2 : s // 2 + 1, :]
            ref[rows, :] = rounded(projected)

        def pair_step(pair, carry, block=block):
            attend_pair(q_ref, k_ref, v_ref, seg_col, seg_row, ctx, lse, block, pair)
            return carry

        lax.fori_loop(0, width // LANES, pair_step, 0)
        own[rows, :] = rounded(dot(ctx[rows, :], g1[:, 3 * width :], 1, 1))
        for k in range(1, n_mp):
            copy = copy_to(
                own.at[rows], recv.at[k - 1, rows], xs.at[block, k - 1], xr.at[block, k - 1],
                {"mp": (x + k) % n_mp},
            )
            copy.start()
            crossing.append(copy)
        relay(z2)
        relay(z3)
    while z2:
        relay(z2)
    for k in range(last):
        relay(z3)
        second.along_y(k)
        second.rest_y(k)
    while z3:
        relay(z3)
    for k in range(last):
        third.along_y(k)
        third.rest_y(k)
    second.arrived()
    third.arrived()
    for copy in crossing:
        copy.wait_recv()
    for gather in (first, second, third):
        gather.finish()
    for copy in crossing:
        copy.wait_send()


def forward(ring, n_mp, tokens, seg_col, seg_row, bias, shards):
    rows, depth = tokens.shape
    width = bias.shape[1]
    blocks = rows // BLOCK
    shape = jax.ShapeDtypeStruct
    gathered = [shape((ring.n * s.shape[0], s.shape[1]), HALF) for s in shards]
    return pl.pallas_call(
        functools.partial(forward_kernel, ring, n_mp),
        name="forward",
        out_shape=gathered
        + [shape((rows, width), HALF)] * 4
        + [shape((rows, LANES), FULL), shape((rows, depth), HALF), shape((n_mp - 1, rows, depth), HALF)],
        in_specs=[VMEM] * 7,
        out_specs=[VMEM, ANY, ANY] + [VMEM] * 7,
        scratch_shapes=Gather.scratch(ring) * 3 + [DMA((blocks, n_mp - 1))] * 2,
        compiler_params=pltpu.CompilerParams(
            collective_id=0, has_side_effects=True, vmem_limit_bytes=48 << 20
        ),
        cost_estimate=pl.CostEstimate(flops=int(2e10), bytes_accessed=int(2e8), transcendentals=0),
    )(tokens, seg_col, seg_row, bias, *shards)


class Scatter:
    def __init__(self, place, grad, out, bufs):
        self.p, self.grad, self.out = place, grad, out
        self.rows = out.shape[0]
        (self.c_in, self.y_in, self.z_in, self.cs, self.cr, self.ys, self.yr, self.zs, self.zr) = bufs
        self.sent, self.c_copy, self.y_copy, self.z_copy = [], {}, {}, {}

    def block(self, z, y, c):
        start = self.p.ring.join(z, y, c) * self.rows
        return self.grad.at[pl.ds(pl.multiple_of(start, self.rows), self.rows)]

    def z_of(self, j):
        return (self.p.z + self.p.ring.outer - j) % self.p.ring.outer

    def y_of(self, i):
        return (self.p.y + self.p.ring.inner - i) % self.p.ring.inner

    def send(self, source, target, send_sem, recv_sem, device):
        copy = copy_to(source, target, send_sem, recv_sem, {"dp": device})
        copy.start()
        self.sent.append(copy)
        return copy

    def order(self):
        outer = self.p.ring.outer
        return [j % outer for j in range(1, outer + 1)]

    def to_core(self, i, j):
        p = self.p
        self.c_copy[i, j] = self.send(
            self.block(self.z_of(j), self.y_of(i), 1 - p.c), self.c_in.at[i, j],
            self.cs.at[i, j], self.cr.at[i, j], p.partner,
        )

    def chip_sum(self, i, j):
        self.c_copy[i, j].wait_recv()
        return self.block(self.z_of(j), self.y_of(i), self.p.c)[...].astype(FULL) + self.c_in[i, j].astype(FULL)

    def along_y(self, i, j):
        total = self.chip_sum(i, j)
        if i > 1:
            self.y_copy[i - 1, j].wait_recv()
            total = total + self.y_in[i - 2, j].astype(FULL)
        self.c_in[i, j] = total.astype(self.c_in.dtype)
        self.y_copy[i, j] = self.send(
            self.c_in.at[i, j], self.y_in.at[i - 1, j],
            self.ys.at[i - 1, j], self.yr.at[i - 1, j], self.p.y_next,
        )

    def along_z(self, j):
        ring = self.p.ring
        total = self.chip_sum(0, j)
        if ring.inner > 1:
            self.y_copy[ring.inner - 1, j].wait_recv()
            total = total + self.y_in[ring.inner - 2, j].astype(FULL)
        step = j if j else ring.outer
        if step > 1:
            self.z_copy[step - 1].wait_recv()
            total = total + self.z_in[step - 2].astype(FULL)
        if j == 0:
            self.out[...] = total
        else:
            self.c_in[0, j] = total.astype(self.c_in.dtype)
            self.z_copy[j] = self.send(
                self.c_in.at[0, j], self.z_in.at[j - 1], self.zs.at[j - 1], self.zr.at[j - 1],
                self.p.z_next,
            )

    def finish(self):
        for copy in self.sent:
            copy.wait_send()

    @staticmethod
    def scratch(ring, rows, columns, dtype):
        z, y = max(ring.outer - 1, 1), max(ring.inner - 1, 1)

        def buf(*lead):
            return pltpu.VMEM((*lead, rows, columns), dtype)

        return [
            buf(ring.inner, ring.outer), buf(y, ring.outer), buf(z),
            DMA((ring.inner, ring.outer)), DMA((ring.inner, ring.outer)),
            DMA((y, ring.outer)), DMA((y, ring.outer)), DMA((z,)), DMA((z,)),
        ]


def spread(terms):
    total = terms[0].astype(FULL)
    for term in terms[1:]:
        total = total + term.astype(FULL)
    return total


def ffn_kernel(terms, aliased, *refs):
    tok, parts, (w_in, w_down, bias, gains, biases) = refs[0], refs[1 : 1 + terms], refs[1 + terms : 6 + terms]
    midh, act, n1, inv1, slope, out, total = refs[6 + terms + aliased :]
    step = pl.program_id(0)

    @pl.when(step == 0)
    def _():
        summed = tok[...].astype(FULL) + spread([p[...] for p in parts]) + biases[2:3, :]
        normed, inv = normalize(summed)
        n1[...] = normed
        inv1[...] = jnp.broadcast_to(inv, inv1.shape)
        midh[...] = rounded(normed * gains[0:1, :] + biases[0:1, :])
        total[...] = jnp.zeros_like(total)

    pre = dot(midh[...], w_in[...]) + bias[...]
    phi = 0.5 * (1.0 + lax.erf(pre * 0.7071067811865476))
    active = rounded(pre * phi)
    act[...] = active
    slope[...] = rounded(phi + pre * jnp.exp(-0.5 * pre * pre) * 0.3989422804014327)
    total[...] += dot(active, w_down[...], 1, 1)

    @pl.when(step == pl.num_programs(0) - 1)
    def _():
        out[...] = rounded(total[...])


def ffn(block, tokens, parts, w_in, w_down, hidden_bias, gains, biases, earlier):
    rows, depth = tokens.shape
    hidden = w_in.shape[1]
    chunk = min(CHUNK, hidden)
    shape = jax.ShapeDtypeStruct
    whole = pl.BlockSpec((BLOCK, depth), lambda j: (block, 0))
    local = pl.BlockSpec((BLOCK, depth), lambda j: (0, 0))
    column = pl.BlockSpec((depth, chunk), lambda j: (0, j))
    fixed = lambda a: pl.BlockSpec(a.shape, lambda j: (0, 0))
    part_specs = [whole if p.shape[0] == rows else local for p in parts]
    n_in = 6 + len(parts)
    return pl.pallas_call(
        functools.partial(ffn_kernel, len(parts), len(earlier)),
        name=f"ffn_{block}",
        grid=(hidden // chunk,),
        out_shape=[
            shape((rows, depth), HALF), shape((rows, hidden), HALF), shape((BLOCK, depth), FULL),
            shape((BLOCK, LANES), FULL), shape((BLOCK, hidden), HALF), shape((BLOCK, depth), HALF),
        ],
        in_specs=[whole] + part_specs
        + [column, column, pl.BlockSpec((1, chunk), lambda j: (0, j)), fixed(gains), fixed(biases)]
        + [ANY] * len(earlier),
        out_specs=[
            whole, pl.BlockSpec((BLOCK, chunk), lambda j: (block, j)), local,
            pl.BlockSpec((BLOCK, LANES), lambda j: (0, 0)), pl.BlockSpec((BLOCK, chunk), lambda j: (0, j)), local,
        ],
        scratch_shapes=[pltpu.VMEM((BLOCK, depth), FULL)],
        input_output_aliases={n_in + i: i for i in range(len(earlier))},
        compiler_params=pltpu.CompilerParams(vmem_limit_bytes=40 << 20),
        cost_estimate=pl.CostEstimate(
            flops=4 * BLOCK * depth * hidden, bytes_accessed=20 << 20, transcendentals=2 * BLOCK * hidden
        ),
    )(tokens, *parts, w_in, w_down, hidden_bias, gains, biases, *earlier)


def ffn_back_kernel(terms, aliased, *refs):
    n1, up, parts = refs[0], refs[1], refs[2 : 2 + terms]
    slope, w_in, w_down, gains, biases = refs[2 + terms : 7 + terms]
    output, gsh, gpreh, gs, sums, pre_sums, out, total = refs[7 + terms + aliased :]
    step = pl.program_id(0)

    @pl.when(step == 0)
    def _():
        middle = n1[...] * gains[0:1, :] + biases[0:1, :]
        second = middle + spread([p[...] for p in parts]) + biases[3:4, :]
        normed, inv = normalize(second)
        output[...] = rounded(normed * gains[1:2, :] + biases[1:2, :])
        upstream = up[...].astype(FULL)
        grad = norm_back(upstream, normed, inv, gains[1:2, :])
        gs[...] = grad
        gsh[...] = rounded(grad)
        sums[...] = jnp.zeros_like(sums)
        sums[0:1, :] = column_sum(upstream * normed)
        sums[1:2, :] = column_sum(upstream)
        sums[2:3, :] = column_sum(grad)
        total[...] = jnp.zeros_like(total)

    grad_pre = dot(gsh[...], w_down[...]) * slope[...].astype(FULL)
    pre_sums[...] = jnp.broadcast_to(column_sum(grad_pre), pre_sums.shape)
    half = rounded(grad_pre)
    gpreh[...] = half
    total[...] += dot(half, w_in[...], 1, 1)

    @pl.when(step == pl.num_programs(0) - 1)
    def _():
        out[...] = rounded(total[...])


def ffn_back(block, n1, grad_output, parts, slope, w_in, w_down, gains, biases, earlier):
    rows, depth = grad_output.shape
    hidden = w_in.shape[1]
    chunk = min(CHUNK, hidden)
    shape = jax.ShapeDtypeStruct
    whole = pl.BlockSpec((BLOCK, depth), lambda j: (block, 0))
    local = pl.BlockSpec((BLOCK, depth), lambda j: (0, 0))
    column = pl.BlockSpec((depth, chunk), lambda j: (0, j))
    fixed = lambda a: pl.BlockSpec(a.shape, lambda j: (0, 0))
    n_in = 7 + len(parts)
    return pl.pallas_call(
        functools.partial(ffn_back_kernel, len(parts), len(earlier)),
        name=f"ffn_back_{block}",
        grid=(hidden // chunk,),
        out_shape=[
            shape((rows, depth), HALF), shape((rows, depth), HALF), shape((rows, hidden), HALF),
            shape((BLOCK, depth), FULL), shape((8, depth), FULL), shape((8, hidden), FULL),
            shape((BLOCK, depth), HALF),
        ],
        in_specs=[local, whole] + [local] * len(parts)
        + [pl.BlockSpec((BLOCK, chunk), lambda j: (0, j)), column, column, fixed(gains), fixed(biases)]
        + [ANY] * len(earlier),
        out_specs=[
            whole, whole, pl.BlockSpec((BLOCK, chunk), lambda j: (block, j)), local,
            pl.BlockSpec((8, depth), lambda j: (0, 0)), pl.BlockSpec((8, chunk), lambda j: (0, j)), local,
        ],
        scratch_shapes=[pltpu.VMEM((BLOCK, depth), FULL)],
        input_output_aliases={n_in + i: i for i in range(len(earlier))},
        compiler_params=pltpu.CompilerParams(vmem_limit_bytes=40 << 20),
        cost_estimate=pl.CostEstimate(
            flops=4 * BLOCK * depth * hidden, bytes_accessed=22 << 20, transcendentals=0
        ),
    )(n1, grad_output, *parts, slope, w_in, w_down, gains, biases, *earlier)


def attend_back_pair(q_ref, k_ref, v_ref, seg_col, seg_row, ctx, lse, gctx, dqkv, small, block, pair):
    rows = pl.ds(block * BLOCK, BLOCK)
    width = q_ref.shape[1]
    start = pl.multiple_of(pair * LANES, LANES)
    lanes = pl.ds(start, LANES)
    keys, values, q = k_ref[rows, lanes], v_ref[rows, lanes], q_ref[rows, lanes]
    queries = q * jnp.asarray(HEAD ** (-0.5), HALF)
    grad = gctx[:, lanes]
    product = grad.astype(FULL) * ctx[rows, lanes].astype(FULL)
    lane = lax.broadcasted_iota(jnp.int32, (BLOCK, LANES), 1)
    same = seg_col[rows, :] == seg_row[pl.ds(block, 1), :]
    per_pair = LANES // HEAD
    log_totals = lse[rows, :]
    grad_q = grad_k = grad_v = jnp.zeros((BLOCK, LANES), FULL)
    for j in range(per_pair):
        mine = (lane // HEAD) == j
        zero = jnp.zeros_like(grad)
        score = jnp.where(same, dot(jnp.where(mine, queries, zero), keys, 1, 1), -1e9)
        log_total = jnp.sum(jnp.where(lane == per_pair * pair + j, log_totals, 0.0), axis=1, keepdims=True)
        delta = jnp.sum(jnp.where(mine, product, 0.0), axis=1, keepdims=True)
        prob = jnp.exp(score - log_total)
        grad_prob = dot(jnp.where(mine, grad, zero), values, 1, 1)
        grad_score = rounded(prob * (grad_prob - delta) * HEAD ** (-0.5))
        grad_q = jnp.where(mine, dot(grad_score, keys), grad_q)
        grad_k = jnp.where(mine, dot(grad_score, q, 0, 0), grad_k)
        grad_v = jnp.where(mine, dot(rounded(prob), grad, 0, 0), grad_v)
    for s, part in enumerate((grad_q, grad_k, grad_v)):
        dqkv[rows, pl.ds(pl.multiple_of(s * width + start, LANES), LANES)] = rounded(part)
    small[6:7, lanes] += column_sum(grad_q)
    small[6:7, pl.ds(pl.multiple_of(width + start, LANES), LANES)] += column_sum(grad_v)


def ffn_weights_kernel(gsh, act, midh, gpreh, down, into):
    down[...] = rounded(dot(gsh[...], act[...], 0, 0))
    into[...] = rounded(dot(midh[...], gpreh[...], 0, 0))


def ffn_weights(gsh, act, midh, gpreh):
    rows, depth = gsh.shape
    hidden = act.shape[1]
    chunk = min(CHUNK, hidden)
    fixed = pl.BlockSpec((rows, depth), lambda j: (0, 0))
    column = pl.BlockSpec((rows, chunk), lambda j: (0, j))
    out = pl.BlockSpec((depth, chunk), lambda j: (0, j))
    return pl.pallas_call(
        ffn_weights_kernel,
        name="ffn_weights",
        grid=(hidden // chunk,),
        out_shape=[jax.ShapeDtypeStruct((depth, hidden), HALF)] * 2,
        in_specs=[fixed, column, fixed, column],
        out_specs=[out, out],
        compiler_params=pltpu.CompilerParams(vmem_limit_bytes=40 << 20),
        cost_estimate=pl.CostEstimate(
            flops=4 * rows * depth * hidden, bytes_accessed=20 << 20, transcendentals=0
        ),
    )(gsh, act, midh, gpreh)


class Total:
    def __init__(self, place, value, stages, inbox, sems):
        self.p, self.value, self.stages, self.inbox = place, value, stages, inbox
        self.ss, self.rs = sems
        self.sent = []

    def stage(self, number, devices, first):
        source = self.value if number == 0 else self.stages.at[number - 1]
        copies = []
        for k, device in enumerate(devices):
            slot = first + k
            copy = copy_to(source, self.inbox.at[slot], self.ss.at[slot], self.rs.at[slot], {"dp": device})
            copy.start()
            copies.append(copy)
        self.sent += copies
        return copies

    def steps(self):
        ring = self.p.ring
        groups = [
            [self.p.partner],
            [self.p.at_y(k) for k in range(1, ring.inner)],
            [self.p.at_z(k) for k in range(1, ring.outer)],
        ]
        first = 0
        for number, devices in enumerate(groups):
            copies = self.stage(number, devices, first)
            yield
            total = (self.value if number == 0 else self.stages.at[number - 1])[...]
            for k, copy in enumerate(copies):
                copy.wait_recv()
                total = total + self.inbox[first + k]
            self.stages[number] = total
            first += len(devices)
        for copy in self.sent:
            copy.wait_send()


def backward_kernel(ring, n_mp, blocks, *refs):
    n_in = 13 + 5 * blocks + (blocks - 1) * n_mp
    ins, refs = list(refs[:n_in]), refs[n_in:]
    take = lambda n: [ins.pop(0) for _ in range(n)]
    g_down, g_in, tokens_h, w1_h, q_h, k_h, v_h, ctx_h = take(8)
    gs_h, n1_h, inv1, sums2, pre = take(blocks), take(blocks), take(blocks), take(blocks), take(blocks)
    parts = [take(n_mp) for _ in range(blocks - 1)]
    back, lse, seg_col, seg_row, gains = take(5)
    out_down, out_in, out_attn, out_small, gsum, own, recv = refs[:7]
    (tok, w1, q, k, v, ctx, gs, n1, gctx, dqkv, gsumh, g_attn, back_in,
     small, stages, inbox) = refs[7:23]
    loads, bs, br, xs, xr, ts, tr = refs[23:30]
    flows_refs = refs[30:]
    per = len(flows_refs) // 3
    place = Place(ring)
    place.enter(n_mp)
    x = lax.axis_index("mp")
    width = q.shape[1]
    depth = gsum.shape[1]

    def load(index, source, target):
        copy = pltpu.make_async_copy(source, target, loads.at[index])
        copy.start()
        return copy

    def load_block(block):
        return [load(8 + block, gs_h[block], gs), load(8 + blocks + block, n1_h[block], n1)]

    crossing = []

    def cross(source, target, send_sems, recv_sems):
        copies = []
        for m in range(1, n_mp):
            copy = copy_to(
                source, target(m - 1), send_sems.at[m - 1], recv_sems.at[m - 1], {"mp": (x + m) % n_mp}
            )
            copy.start()
            copies.append(copy)
        crossing.extend(copies)
        return copies

    arriving = cross(back, lambda m: back_in.at[m], bs, br)
    block_loads = load_block(0)
    w_load = load(0, w1_h, w1)
    qkv_loads = [load(1 + i, a, b) for i, (a, b) in enumerate(((q_h, q), (k_h, k), (v_h, v), (ctx_h, ctx)))]
    tok_load = load(5, tokens_h, tok)
    down, into, attn = (
        Scatter(place, g, o, flows_refs[i * per : (i + 1) * per])
        for i, (g, o) in enumerate(((g_down, out_down), (g_in, out_in), (g_attn, out_attn)))
    )
    order = down.order()
    inner = [i % ring.inner for i in range(1, ring.inner + 1)]

    def send_core(flow):
        for i in inner:
            for j in order:
                flow.to_core(i, j)

    def send_y(flow):
        for i in inner[:-1]:
            for j in order:
                flow.along_y(i, j)

    send_core(down)
    send_core(into)
    later = [functools.partial(down.along_z, j) for j in order]
    later += [functools.partial(into.along_z, j) for j in order]
    small[...] = jnp.zeros_like(small)
    for block in range(blocks):
        small[3:6, :] += sums2[block][0:3, :]
        for r in range(pre[block].shape[1] // depth):
            small[7 + r : 8 + r, :] += pre[block][0:1, r * depth : (r + 1) * depth]

    send_y(down)
    for block in range(blocks):
        rows = pl.ds(block * BLOCK, BLOCK)
        for copy in block_loads:
            copy.wait()
        if block == blocks - 1:
            for copy in arriving:
                copy.wait_recv()
            terms = [back[...]] + [back_in[m] for m in range(n_mp - 1)]
        else:
            terms = [p[...] for p in parts[block]]
        normed = n1[...]
        grad_middle = gs[...] + spread(terms)
        grad = norm_back(grad_middle, normed, inv1[block][:, 0:1], gains[0:1, :])
        gs[...] = grad
        gsumh[rows, :] = rounded(grad)
        saving = pltpu.make_async_copy(gs, gsum.at[rows], loads.at[6])
        saving.start()
        small[0:1, :] += column_sum(grad_middle * normed)
        small[1:2, :] += column_sum(grad_middle)
        small[2:3, :] += column_sum(grad)
        if block == 0:
            w_load.wait()
        gctx[...] = rounded(dot(gsumh[rows, :], w1[:, 3 * width :]))
        if block == 0:
            send_y(into)
            for copy in qkv_loads:
                copy.wait()
        elif later:
            later.pop(0)()
        saving.wait()
        if block + 1 < blocks:
            block_loads = load_block(block + 1)

        def pair_step(pair, carry, block=block):
            attend_back_pair(q, k, v, seg_col, seg_row, ctx, lse, gctx, dqkv, small, block, pair)
            return carry

        lax.fori_loop(0, width // LANES, pair_step, 0)
        total = None
        for s in range(3):
            part = slice(s * width, (s + 1) * width)
            term = dot(dqkv[rows, part], w1[:, part], 1, 1)
            total = term if total is None else total + term
        own[rows, :] = rounded(total)
        cross(own.at[rows], lambda m: recv.at[m, rows], xs.at[block], xr.at[block])
        if later:
            later.pop(0)()
    summing = Total(place, small, stages, inbox, (ts, tr)).steps()
    next(summing)
    tok_load.wait()
    for s in range(3):
        part = slice(s * width, (s + 1) * width)
        g_attn[:, part] = rounded(dot(tok[...], dqkv[:, part], 0, 0))
    g_attn[:, 3 * width :] = rounded(dot(gsumh[...], ctx[...], 0, 0))
    send_core(attn)
    for _ in summing:
        if later:
            later.pop(0)()
    out_small[...] = stages[2]
    send_y(attn)
    while later:
        later.pop(0)()
    for j in order:
        attn.along_z(j)
    for flow in (down, into, attn):
        flow.finish()
    for copy in crossing[n_mp - 1 :]:
        copy.wait_recv()
    for copy in crossing:
        copy.wait_send()


def backward(ring, n_mp, grads, tokens, w1, qkvc, saved, lse, seg_col, seg_row, gains):
    rows, depth = tokens.shape
    width = qkvc[0].shape[1]
    blocks = len(saved)
    shape = jax.ShapeDtypeStruct
    ffn_rows, hidden = grads[0].shape[0] // ring.n, grads[0].shape[1]
    small_rows = 8 * pl.cdiv(7 + hidden // depth, 8)
    peers = ring.core - 1 + ring.inner - 1 + ring.outer - 1
    column = lambda name: [s[name] for s in saved]
    parts = [p for s in saved[:-1] for p in s["back"]]
    operands = [*grads, tokens, w1, *qkvc, *column("gs"), *column("n1"), *column("inv1"),
                *column("sums2"), *column("pre"), *parts, saved[-1]["term"], lse, seg_col, seg_row, gains]
    specs = [VMEM] * 2 + [ANY] * 6 + [ANY] * (2 * blocks) + [VMEM] * (3 * blocks + len(parts) + 5)
    flow = Scatter.scratch(ring, ffn_rows, hidden, HALF)
    half = lambda *dims: pltpu.VMEM(dims, HALF)
    full = lambda *dims: pltpu.VMEM(dims, FULL)
    return pl.pallas_call(
        functools.partial(backward_kernel, ring, n_mp, blocks),
        name="backward",
        out_shape=[shape((ffn_rows, hidden), FULL)] * 2
        + [shape((ffn_rows, 4 * width), FULL), shape((small_rows, depth), FULL),
           shape((rows, depth), FULL), shape((rows, depth), HALF), shape((n_mp - 1, rows, depth), HALF)],
        in_specs=specs,
        out_specs=[VMEM] * 4 + [ANY] + [VMEM] * 2,
        scratch_shapes=[
            half(rows, depth), half(*w1.shape), *[half(rows, width)] * 4,
            full(BLOCK, depth), full(BLOCK, depth), half(BLOCK, width), half(rows, 3 * width),
            half(rows, depth), half(depth, 4 * width), half(n_mp - 1, BLOCK, depth),
            full(small_rows, depth), full(3, small_rows, depth), full(peers, small_rows, depth),
            DMA((8 + 2 * blocks,)), DMA((n_mp - 1,)), DMA((n_mp - 1,)),
            DMA((blocks, n_mp - 1)), DMA((blocks, n_mp - 1)), DMA((peers,)), DMA((peers,)),
            *flow, *flow, *Scatter.scratch(ring, ffn_rows, 4 * width, HALF),
        ],
        compiler_params=pltpu.CompilerParams(
            collective_id=1, has_side_effects=True, vmem_limit_bytes=67043328
        ),
        cost_estimate=pl.CostEstimate(flops=int(4e10), bytes_accessed=int(2e8), transcendentals=0),
    )(*operands)


def across(term, n_mp):
    shifts = [[(i, (i + k) % n_mp) for i in range(n_mp)] for k in range(1, n_mp)]
    return [term] + [lax.ppermute(term, "mp", shift) for shift in shifts]


def per_device(
    n_dp, n_mp,
    tokens, segments, grad_output, w_qkv, w_out, w_in, w_down, qv_bias, ffn_bias, gains, biases
):
    ring = Ring(n_dp)
    width = w_qkv.shape[2]
    rows, depth = tokens.shape
    piece = depth // n_dp
    n_heads = width // HEAD
    blocks = range(rows // BLOCK)

    shards = [jnp.concatenate([w_qkv[0], w_qkv[1], w_qkv[2], w_out.T], axis=1), w_in, w_down.T]
    seg_col = segments.reshape(rows, 1)
    seg_row = segments.reshape(-1, BLOCK)
    w1, w2, w3, q, k, v, ctx, lse, own, recv = forward(
        ring, n_mp, tokens, seg_col, seg_row, qv_bias.reshape(2, width), shards
    )
    attended = [own] + [recv[i] for i in range(n_mp - 1)]
    hidden_bias = ffn_bias.reshape(1, -1)

    saved, earlier = [], []
    for block in blocks:
        midh, act, n1, inv1, slope, term = ffn(
            block, tokens, attended, w2, w3, hidden_bias, gains, biases, earlier
        )
        earlier = [midh, act]
        saved.append(dict(n1=n1, inv1=inv1, slope=slope, ffn=across(term, n_mp)))
    earlier = []
    for block, s in zip(blocks, saved):
        output, gsh, gpreh, s["gs"], s["sums2"], s["pre"], term = ffn_back(
            block, s["n1"], grad_output, s["ffn"], s["slope"], w2, w3, gains, biases, earlier
        )
        earlier = [output, gsh, gpreh]
        s["term"] = term
        if block + 1 < len(saved):
            s["back"] = across(term, n_mp)
    grads = ffn_weights(gsh, act, midh, gpreh)
    grad_down, grad_in, grad_attn, small, gsum, own, recv = backward(
        ring, n_mp, grads, tokens, w1, (q, k, v, ctx), saved, lse, seg_col, seg_row, gains
    )
    grad_tokens = gsum + spread([own] + [recv[i] for i in range(n_mp - 1)])

    me = lax.axis_index("dp")
    bit = HEAD // n_dp
    norms = lax.dynamic_slice(small, (0, me * piece), (6, piece))
    heads = lax.dynamic_slice(small[6, : 2 * width].reshape(2, n_heads, HEAD), (0, 0, me * bit), (2, n_heads, bit))
    hidden = w_in.shape[1]
    pre = small[7 : 7 + hidden // depth].reshape(-1, HEAD)
    return (
        output,
        grad_tokens,
        jnp.stack([grad_attn[:, s * width : (s + 1) * width] for s in range(3)]),
        grad_attn[:, 3 * width :].T,
        grad_in,
        grad_down.T,
        heads,
        lax.dynamic_slice(pre, (0, me * bit), (hidden // HEAD, bit)),
        jnp.stack([norms[0], norms[3]]),
        jnp.stack([norms[1], norms[4], norms[2], norms[5]]),
    )


def solution(mesh):
    n_dp, n_mp = mesh.shape["dp"], mesh.shape["mp"]
    placed = (
        P("dp", None),
        P("dp"),
        P("dp", None),
        P(None, "dp", "mp"),
        P("mp", "dp"),
        P("dp", "mp"),
        P("mp", "dp"),
        P(None, "mp", None),
        P("mp", None),
        P(),
        P(),
    )

    def body(*args):
        return per_device(n_dp, n_mp, *args)

    return jax.shard_map(
        body,
        mesh=mesh,
        in_specs=placed,
        out_specs=(
            P("dp", None),
            P("dp", None),
            P(None, "dp", "mp"),
            P("mp", "dp"),
            P("dp", "mp"),
            P("mp", "dp"),
            P(None, "mp", "dp"),
            P("mp", "dp"),
            P(None, "dp"),
            P(None, "dp"),
        ),
        check_vma=False,
    )
```

```python
import functools

import jax
import jax.numpy as jnp
from jax import lax
from jax.experimental import pallas as pl
from jax.experimental.pallas import tpu as pltpu
from jax.sharding import PartitionSpec as P

HEAD = 64
BLOCK = 512
CORES = 2
OUTER = 4
LANES = 128
CHUNK = 512

EPS = 1e-05
HALF = jnp.bfloat16
FULL = jnp.float32
MESH = pl.DeviceIdType.MESH
VMEM = pl.BlockSpec(memory_space=pltpu.VMEM)
ANY = pl.BlockSpec(memory_space=pl.ANY)
DMA = pltpu.SemaphoreType.DMA


def rounded(value):
    return value.astype(HALF)


def dot(left, right, left_dim=1, right_dim=0):
    return lax.dot_general(
        left, right, (((left_dim,), (right_dim,)), ((), ())), preferred_element_type=FULL
    )


def normalize(summed):
    centered = summed - jnp.mean(summed, axis=-1, keepdims=True)
    inv_std = lax.rsqrt(jnp.mean(centered * centered, axis=-1, keepdims=True) + EPS)
    return (centered * inv_std, inv_std)


def norm_back(grad_in, normed, inv_std, gain):
    scaled = grad_in * gain
    return inv_std * (
        scaled
        - jnp.mean(scaled, axis=-1, keepdims=True)
        - normed * jnp.mean(scaled * normed, axis=-1, keepdims=True)
    )


def column_sum(value):
    return jnp.sum(value, axis=0, keepdims=True)


class Ring:
    def __init__(self, n_dp):
        self.n = n_dp
        self.core = CORES
        self.outer = OUTER if n_dp % (OUTER * CORES) == 0 else 1
        self.inner = n_dp // (self.outer * self.core)

    def split(self, index):
        return index // (self.inner * self.core), (index // self.core) % self.inner, index % self.core

    def join(self, outer, inner, core):
        return (outer * self.inner + inner) * self.core + core


class Place:
    def __init__(self, ring):
        self.ring = ring
        self.z, self.y, self.c = ring.split(lax.axis_index("dp"))
        self.z_next = ring.join((self.z + 1) % ring.outer, self.y, self.c)
        self.z_last = ring.join((self.z + ring.outer - 1) % ring.outer, self.y, self.c)
        self.y_next = ring.join(self.z, (self.y + 1) % ring.inner, self.c)
        self.y_last = ring.join(self.z, (self.y + ring.inner - 1) % ring.inner, self.c)
        self.partner = ring.join(self.z, self.y, 1 - self.c)

    def at_z(self, k):
        return self.ring.join((self.z + k) % self.ring.outer, self.y, self.c)

    def at_y(self, k):
        return self.ring.join(self.z, (self.y + k) % self.ring.inner, self.c)

    def enter(self, n_mp=1):
        peers = [{"dp": self.partner}]
        peers += [{"dp": self.at_z(k)} for k in range(1, self.ring.outer)]
        peers += [{"dp": self.at_y(k)} for k in range(1, self.ring.inner)]
        x = lax.axis_index("mp")
        peers += [{"mp": (x + k) % n_mp} for k in range(1, n_mp)]
        barrier = pltpu.get_barrier_semaphore()
        for peer in peers:
            pl.semaphore_signal(barrier, inc=1, device_id=peer, device_id_type=MESH)
        pl.semaphore_wait(barrier, len(peers))


def copy_to(source, target, send_sem, recv_sem, device):
    return pltpu.make_async_remote_copy(
        src_ref=source, dst_ref=target, send_sem=send_sem, recv_sem=recv_sem,
        device_id=device, device_id_type=MESH,
    )


class Gather:
    def __init__(self, place, shard, out, sems):
        self.p, self.shard, self.out = place, shard, out
        self.own_sem, self.zs, self.zr, self.ys, self.yr, self.cs, self.cr = sems
        self.rows = shard.shape[0]
        self.sent, self.z_in, self.y_in, self.c_in = [], {}, {}, []
        self.own = pltpu.make_async_copy(shard, self.at(place.z, place.y, place.c), self.own_sem)

    def at(self, z, y, c):
        start = self.p.ring.join(z, y, c) * self.rows
        return self.out.at[pl.ds(pl.multiple_of(start, self.rows), self.rows)]

    def send(self, source, target, send_sem, recv_sem, device):
        copy = copy_to(source, target, send_sem, recv_sem, {"dp": device})
        copy.start()
        self.sent.append(copy)
        return copy

    def along_z(self, k):
        p, ring = self.p, self.p.ring
        target = self.at((p.z + ring.outer - k) % ring.outer, p.y, p.c)
        source = target
        if k == 0:
            self.own.start()
            source = self.shard
        else:
            self.z_in[k].wait_recv()
        if k < ring.outer - 1:
            self.z_in[k + 1] = self.send(source, target, self.zs.at[k], self.zr.at[k], p.z_next)
        if ring.inner > 1:
            self.y_in[k, 1] = self.send(source, target, self.ys.at[k, 0], self.yr.at[k, 0], p.y_next)
        self.c_in.append(self.send(source, target, self.cs.at[k, 0], self.cr.at[k, 0], p.partner))

    def along_y(self, k, step=1):
        p, ring = self.p, self.p.ring
        if step >= ring.inner:
            return
        target = self.at((p.z + ring.outer - k) % ring.outer, (p.y + ring.inner - step) % ring.inner, p.c)
        self.y_in[k, step].wait_recv()
        if step < ring.inner - 1:
            self.y_in[k, step + 1] = self.send(
                target, target, self.ys.at[k, step], self.yr.at[k, step], p.y_next
            )
        self.c_in.append(
            self.send(target, target, self.cs.at[k, step], self.cr.at[k, step], p.partner)
        )

    def rest_y(self, k):
        for step in range(2, self.p.ring.inner):
            self.along_y(k, step)

    def arrived(self):
        for copy in self.c_in:
            copy.wait_recv()
        self.own.wait()

    def finish(self):
        for copy in self.sent:
            copy.wait_send()

    @staticmethod
    def scratch(ring):
        z, y = max(ring.outer - 1, 1), max(ring.inner - 1, 1)
        return [
            DMA, DMA((z,)), DMA((z,)), DMA((ring.outer, y)), DMA((ring.outer, y)),
            DMA((ring.outer, ring.inner)), DMA((ring.outer, ring.inner)),
        ]


def attend_pair(qkvc, seg_col, seg_row, lse_ref, block, pair):
    width = qkvc.shape[1] // 4
    rows = pl.ds(block * BLOCK, BLOCK)

    def lanes(member):
        return pl.ds(pl.multiple_of(member * width + pair * LANES, LANES), LANES)

    queries = qkvc[rows, lanes(0)] * jnp.asarray(HEAD ** (-0.5), HALF)
    keys, values = qkvc[rows, lanes(1)], qkvc[rows, lanes(2)]
    lane = lax.broadcasted_iota(jnp.int32, (BLOCK, LANES), 1)
    same = seg_col[rows, :] == seg_row[pl.ds(block, 1), :]
    per_pair = LANES // HEAD
    context = jnp.zeros((BLOCK, LANES), FULL)
    log_totals = lse_ref[rows, :]
    for j in range(per_pair):
        mine = (lane // HEAD) == j
        score = jnp.where(same, dot(jnp.where(mine, queries, jnp.zeros_like(queries)), keys, 1, 1), -1e9)
        top = jnp.max(score, axis=1, keepdims=True)
        exps = jnp.exp(score - top)
        total = jnp.sum(exps, axis=1, keepdims=True)
        weights = rounded(exps * (1.0 / total))
        context = jnp.where(mine, dot(weights, values), context)
        log_totals = jnp.where(lane == per_pair * pair + j, top + jnp.log(total), log_totals)
    lse_ref[rows, :] = log_totals
    qkvc[rows, lanes(3)] = rounded(context)


def over_columns(columns, body):
    chunk = min(CHUNK, columns)

    def step(j, carry):
        body(pl.ds(pl.multiple_of(j * chunk, chunk), chunk))
        return carry

    lax.fori_loop(0, columns // chunk, step, 0)


def spread(terms):
    total = terms[0].astype(FULL)
    for term in terms[1:]:
        total = total + term.astype(FULL)
    return total


class Cross:
    def __init__(self, n_mp):
        self.n_mp, self.x = n_mp, lax.axis_index("mp")

    def send(self, source, target, send_sems, recv_sems):
        copies = []
        for m in range(1, self.n_mp):
            copy = copy_to(
                source, target(m - 1), send_sems.at[m - 1], recv_sems.at[m - 1],
                {"mp": (self.x + m) % self.n_mp},
            )
            copy.start()
            copies.append(copy)
        return copies


def received(copies):
    for copy in copies:
        copy.wait_recv()


def forward_kernel(ring, n_mp, *refs):
    tok, seg_col, seg_row, bias, s1, s2, s3, hidden_bias, gains, biases = refs[:10]
    g1, g2, g3, qkvc_out, act_out, slope_out, midh_out, n1_out, own_out, recv_out, lse, inv1 = refs[10:22]
    w1, w2, w3, qkvc, own, recv, act, slope, midh, n1, term, term_in = refs[22:34]
    stores, xs, xr, fs, fr = refs[34:39]
    sems = refs[39:]
    per = len(sems) // 3
    place = Place(ring)
    place.enter(n_mp)
    cross = Cross(n_mp)
    first, second, third = (
        Gather(place, s, g, sems[i * per : (i + 1) * per])
        for i, (s, g) in enumerate(((s1, w1), (s2, w2), (s3, w3)))
    )
    width = qkvc.shape[1] // 4
    depth, hidden = tok.shape[1], act.shape[1]
    blocks = tok.shape[0] // BLOCK
    saving = []

    def save(source, target):
        copy = pltpu.make_async_copy(source, target, stores.at[len(saving)])
        copy.start()
        saving.append(copy)

    last = ring.outer
    for k in range(last):
        first.along_z(k)
        if k >= 1:
            first.along_y(k - 1)
    second.along_z(0)
    first.along_y(last - 1)
    for k in range(last):
        first.rest_y(k)
    z2 = [functools.partial(second.along_z, k) for k in range(1, last)]
    z3 = [functools.partial(third.along_z, k) for k in range(last)]
    first.arrived()
    lse[...] = jnp.zeros_like(lse)

    def relay(steps):
        if steps:
            steps.pop(0)()

    relay(z2)
    crossing, attended, ffn_terms = [], [], []
    for block in range(blocks):
        rows = pl.ds(block * BLOCK, BLOCK)

        def project(s, carry, rows=rows):
            part = pl.ds(pl.multiple_of(s * width, width), width)
            qkvc[rows, part] = rounded(dot(tok[rows, :], w1[:, part]) + bias[pl.ds(s, 1), :])
            return carry

        lax.fori_loop(0, 3, project, 0)

        def pair_step(pair, carry, block=block):
            attend_pair(qkvc, seg_col, seg_row, lse, block, pair)
            return carry

        lax.fori_loop(0, width // LANES, pair_step, 0)
        own[rows, :] = rounded(dot(qkvc[rows, 3 * width :], w1[:, 3 * width :], 1, 1))
        attended.append(cross.send(own.at[rows], lambda m: recv.at[m, rows], xs.at[block], xr.at[block]))
        relay(z2)
        relay(z3)
    save(w1, g1)
    save(qkvc, qkvc_out)
    while z2:
        relay(z2)
    for k in range(last):
        relay(z3)
        second.along_y(k)
        second.rest_y(k)
    while z3:
        relay(z3)
    second.arrived()
    save(w2, g2)
    for block in range(blocks):
        rows = pl.ds(block * BLOCK, BLOCK)
        received(attended[block])
        crossing += attended[block]
        terms = [own[rows, :]] + [recv[m, rows, :] for m in range(n_mp - 1)]
        summed = tok[rows, :].astype(FULL) + spread(terms) + biases[2:3, :]
        normed, inv = normalize(summed)
        n1[rows, :] = normed
        inv1[rows, :] = jnp.broadcast_to(inv, (BLOCK, LANES))
        midh[rows, :] = rounded(normed * gains[0:1, :] + biases[0:1, :])

        def up(part, rows=rows):
            pre = dot(midh[rows, :], w2[:, part]) + hidden_bias[:, part]
            phi = 0.5 * (1.0 + lax.erf(pre * 0.7071067811865476))
            act[rows, part] = rounded(pre * phi)
            slope[rows, part] = rounded(phi + pre * jnp.exp(-0.5 * pre * pre) * 0.3989422804014327)

        over_columns(hidden, up)
        if block == 0:
            for k in range(last):
                third.along_y(k)
                third.rest_y(k)
            third.arrived()
            save(w3, g3)

        def down(part, rows=rows):
            term[rows, part] = rounded(dot(act[rows, :], w3[part, :], 1, 1))

        over_columns(depth, down)
        if block + 1 < blocks:
            ffn_terms.append(
                cross.send(term.at[rows], lambda m: term_in.at[m, rows], fs.at[block], fr.at[block])
            )
    save(act, act_out)
    save(slope, slope_out)
    save(midh, midh_out)
    save(n1, n1_out)
    save(term, own_out)
    for copies in ffn_terms:
        received(copies)
        crossing += copies
    save(term_in, recv_out)
    for gather in (first, second, third):
        gather.finish()
    for copy in crossing:
        copy.wait_send()
    for copy in saving:
        copy.wait()


def forward(ring, n_mp, tokens, seg_col, seg_row, bias, shards, hidden_bias, gains, biases):
    rows, depth = tokens.shape
    width, hidden = bias.shape[1], hidden_bias.shape[1]
    blocks = rows // BLOCK
    shape = jax.ShapeDtypeStruct
    gathered = [(ring.n * s.shape[0], s.shape[1]) for s in shards]
    early = (blocks - 1) * BLOCK
    kept = [
        *((dims, HALF) for dims in gathered), ((rows, 4 * width), HALF), ((rows, hidden), HALF),
        ((rows, hidden), HALF), ((rows, depth), HALF), ((rows, depth), FULL), ((rows, depth), HALF),
        ((n_mp - 1, early, depth), HALF),
    ]
    scratch = [pltpu.VMEM(dims, kind) for dims, kind in kept]
    partial = [pltpu.VMEM((rows, depth), HALF), pltpu.VMEM((n_mp - 1, rows, depth), HALF)]
    return pl.pallas_call(
        functools.partial(forward_kernel, ring, n_mp),
        name="forward",
        out_shape=[shape(dims, kind) for dims, kind in kept] + [shape((rows, LANES), FULL)] * 2,
        in_specs=[VMEM] * 10,
        out_specs=[ANY] * len(kept) + [VMEM] * 2,
        scratch_shapes=scratch[:4] + partial + scratch[4:]
        + [DMA((len(kept),))] + [DMA((blocks, n_mp - 1))] * 4 + Gather.scratch(ring) * 3,
        compiler_params=pltpu.CompilerParams(
            collective_id=0, has_side_effects=True, vmem_limit_bytes=60 << 20
        ),
        cost_estimate=pl.CostEstimate(flops=int(2e10), bytes_accessed=int(2e8), transcendentals=0),
    )(tokens, seg_col, seg_row, bias, *shards, hidden_bias, gains, biases)


class Scatter:
    def __init__(self, place, grad, out, bufs):
        self.p, self.grad, self.out = place, grad, out
        self.rows = out.shape[0]
        (self.c_in, self.y_in, self.z_in, self.cs, self.cr, self.ys, self.yr, self.zs, self.zr) = bufs
        self.sent, self.c_copy, self.y_copy, self.z_copy = [], {}, {}, {}

    def block(self, z, y, c):
        start = self.p.ring.join(z, y, c) * self.rows
        return self.grad.at[pl.ds(pl.multiple_of(start, self.rows), self.rows)]

    def z_of(self, j):
        return (self.p.z + self.p.ring.outer - j) % self.p.ring.outer

    def y_of(self, i):
        return (self.p.y + self.p.ring.inner - i) % self.p.ring.inner

    def send(self, source, target, send_sem, recv_sem, device):
        copy = copy_to(source, target, send_sem, recv_sem, {"dp": device})
        copy.start()
        self.sent.append(copy)
        return copy

    def order(self):
        outer = self.p.ring.outer
        return [j % outer for j in range(1, outer + 1)]

    def to_core(self, i, j):
        p = self.p
        self.c_copy[i, j] = self.send(
            self.block(self.z_of(j), self.y_of(i), 1 - p.c), self.c_in.at[i, j],
            self.cs.at[i, j], self.cr.at[i, j], p.partner,
        )

    def chip_sum(self, i, j):
        self.c_copy[i, j].wait_recv()
        return self.block(self.z_of(j), self.y_of(i), self.p.c)[...].astype(FULL) + self.c_in[i, j].astype(FULL)

    def along_y(self, i, j):
        total = self.chip_sum(i, j)
        if i > 1:
            self.y_copy[i - 1, j].wait_recv()
            total = total + self.y_in[i - 2, j].astype(FULL)
        self.c_in[i, j] = total.astype(self.c_in.dtype)
        self.y_copy[i, j] = self.send(
            self.c_in.at[i, j], self.y_in.at[i - 1, j],
            self.ys.at[i - 1, j], self.yr.at[i - 1, j], self.p.y_next,
        )

    def along_z(self, j):
        ring = self.p.ring
        total = self.chip_sum(0, j)
        if ring.inner > 1:
            self.y_copy[ring.inner - 1, j].wait_recv()
            total = total + self.y_in[ring.inner - 2, j].astype(FULL)
        step = j if j else ring.outer
        if step > 1:
            self.z_copy[step - 1].wait_recv()
            total = total + self.z_in[step - 2].astype(FULL)
        if j == 0:
            self.out[...] = total
        else:
            self.c_in[0, j] = total.astype(self.c_in.dtype)
            self.z_copy[j] = self.send(
                self.c_in.at[0, j], self.z_in.at[j - 1], self.zs.at[j - 1], self.zr.at[j - 1],
                self.p.z_next,
            )

    def finish(self):
        for copy in self.sent:
            copy.wait_send()

    @staticmethod
    def scratch(ring, rows, columns, dtype):
        z, y = max(ring.outer - 1, 1), max(ring.inner - 1, 1)

        def buf(*lead):
            return pltpu.VMEM((*lead, rows, columns), dtype)

        return [
            buf(ring.inner, ring.outer), buf(y, ring.outer), buf(z),
            DMA((ring.inner, ring.outer)), DMA((ring.inner, ring.outer)),
            DMA((y, ring.outer)), DMA((y, ring.outer)), DMA((z,)), DMA((z,)),
        ]


def attend_back_pair(qkvc, seg_col, seg_row, lse, gctx, dqkv, small, block, pair):
    rows = pl.ds(block * BLOCK, BLOCK)
    width = qkvc.shape[1] // 4

    def lanes(member):
        return pl.ds(pl.multiple_of(member * width + pair * LANES, LANES), LANES)

    q, keys, values = qkvc[rows, lanes(0)], qkvc[rows, lanes(1)], qkvc[rows, lanes(2)]
    queries = q * jnp.asarray(HEAD ** (-0.5), HALF)
    grad = gctx[:, lanes(0)]
    product = grad.astype(FULL) * qkvc[rows, lanes(3)].astype(FULL)
    lane = lax.broadcasted_iota(jnp.int32, (BLOCK, LANES), 1)
    same = seg_col[rows, :] == seg_row[pl.ds(block, 1), :]
    per_pair = LANES // HEAD
    log_totals = lse[rows, :]
    grad_q = grad_k = grad_v = jnp.zeros((BLOCK, LANES), FULL)
    for j in range(per_pair):
        mine = (lane // HEAD) == j
        zero = jnp.zeros_like(grad)
        score = jnp.where(same, dot(jnp.where(mine, queries, zero), keys, 1, 1), -1e9)
        log_total = jnp.sum(jnp.where(lane == per_pair * pair + j, log_totals, 0.0), axis=1, keepdims=True)
        delta = jnp.sum(jnp.where(mine, product, 0.0), axis=1, keepdims=True)
        prob = jnp.exp(score - log_total)
        grad_prob = dot(jnp.where(mine, grad, zero), values, 1, 1)
        grad_score = rounded(prob * (grad_prob - delta) * HEAD ** (-0.5))
        grad_q = jnp.where(mine, dot(grad_score, keys), grad_q)
        grad_k = jnp.where(mine, dot(grad_score, q, 0, 0), grad_k)
        grad_v = jnp.where(mine, dot(rounded(prob), grad, 0, 0), grad_v)
    for member, part in enumerate((grad_q, grad_k, grad_v)):
        dqkv[rows, lanes(member)] = rounded(part)
    small[6:7, lanes(0)] += column_sum(grad_q)
    small[6:7, lanes(1)] += column_sum(grad_v)


class Total:
    def __init__(self, place, value, stages, inbox, sems):
        self.p, self.value, self.stages, self.inbox = place, value, stages, inbox
        self.ss, self.rs = sems
        self.sent = []

    def stage(self, number, devices, first):
        source = self.value if number == 0 else self.stages.at[number - 1]
        copies = []
        for k, device in enumerate(devices):
            slot = first + k
            copy = copy_to(source, self.inbox.at[slot], self.ss.at[slot], self.rs.at[slot], {"dp": device})
            copy.start()
            copies.append(copy)
        self.sent += copies
        return copies

    def steps(self):
        ring = self.p.ring
        groups = [
            [self.p.partner],
            [self.p.at_y(k) for k in range(1, ring.inner)],
            [self.p.at_z(k) for k in range(1, ring.outer)],
        ]
        first = 0
        for number, devices in enumerate(groups):
            copies = self.stage(number, devices, first)
            yield
            total = (self.value if number == 0 else self.stages.at[number - 1])[...]
            for k, copy in enumerate(copies):
                copy.wait_recv()
                total = total + self.inbox[first + k]
            self.stages[number] = total
            first += len(devices)
        for copy in self.sent:
            copy.wait_send()


def backward_kernel(ring, n_mp, *refs):
    (w1_h, w2_h, w3_h, qkvc_h, act_h, slope_h, midh_h, n1_h, term_h, recv_h, tokens_h, up_h,
     lse, inv1, seg_col, seg_row, gains, biases) = refs[:18]
    out_down, out_in, out_attn, out_small, output, grad_tokens, own, recv = refs[18:26]
    (weights, g_down, g_in, g_attn, qkvc, tok, gsumh, dqkv, n1, gs, up, term_in, last_in, back_in,
     gctx, small, pre_sums, stages, inbox) = refs[26:45]
    loads, ls, lr, bs, br, xs, xr, ts, tr = refs[45:54]
    flows_refs = refs[54:]
    per = len(flows_refs) // 3
    act, gsh, midh, gpreh = qkvc, tok, gsumh, g_attn
    place = Place(ring)
    place.enter(n_mp)
    cross = Cross(n_mp)
    rows_all, depth = own.shape
    width, hidden = qkvc.shape[1] // 4, g_attn.shape[1]
    blocks = rows_all // BLOCK
    rows_of = [pl.ds(block * BLOCK, BLOCK) for block in range(blocks)]
    used = []

    def load(source, target):
        copy = pltpu.make_async_copy(source, target, loads.at[len(used)])
        used.append(copy)
        copy.start()
        return copy

    def load_rows(block):
        rows = rows_of[block]
        copies = [load(n1_h.at[rows], n1), load(up_h.at[rows], up), load(term_h.at[rows], own.at[rows])]
        if block + 1 < blocks:
            copies.append(load(recv_h.at[:, rows], term_in))
        return copies

    last = rows_of[-1]
    last_copies = cross.send(term_h.at[last], lambda m: last_in.at[m], ls, lr)
    row_loads = load_rows(0)
    w3_load = load(w3_h, weights)
    slope_load = load(slope_h, gpreh)
    w2_load = load(w2_h, g_in)
    act_load = load(act_h, act)
    midh_load = load(midh_h, midh)
    small[...] = jnp.zeros_like(small)
    pre_sums[...] = jnp.zeros_like(pre_sums)
    crossing, backs = list(last_copies), []
    for block, rows in enumerate(rows_of):
        for copy in row_loads:
            copy.wait()
        if block == blocks - 1:
            received(last_copies)
            others = [last_in[m] for m in range(n_mp - 1)]
        else:
            others = [term_in[m] for m in range(n_mp - 1)]
        middle = n1[...] * gains[0:1, :] + biases[0:1, :]
        second = middle + spread([own[rows, :]] + others) + biases[3:4, :]
        normed, inv = normalize(second)
        upstream = up[...].astype(FULL)
        grad = norm_back(upstream, normed, inv, gains[1:2, :])
        small[3:4, :] += column_sum(upstream * normed)
        small[4:5, :] += column_sum(upstream)
        small[5:6, :] += column_sum(grad)
        up[...] = rounded(normed * gains[1:2, :] + biases[1:2, :])
        gs[...] = grad
        gsh[rows, :] = rounded(grad)
        saving = [load(up, output.at[rows]), load(gs, grad_tokens.at[rows])]
        if block == 0:
            w3_load.wait()
            slope_load.wait()

        def to_hidden(part, rows=rows):
            grad_pre = dot(gsh[rows, :], weights[:, part]) * gpreh[rows, part].astype(FULL)
            pre_sums[0:1, part] += column_sum(grad_pre)
            gpreh[rows, part] = rounded(grad_pre)

        over_columns(hidden, to_hidden)
        for copy in saving:
            copy.wait()
        if block + 1 < blocks:
            row_loads = load_rows(block + 1)
        else:
            w1_load = load(w1_h, weights)
        if block == 0:
            w2_load.wait()

        def to_model(part, rows=rows):
            own[rows, part] = rounded(dot(gpreh[rows, :], g_in[part, :], 1, 1))

        over_columns(depth, to_model)
        backs.append(cross.send(own.at[rows], lambda m: back_in.at[m, rows], bs.at[block], br.at[block]))
    for r in range(hidden // depth):
        small[7 + r : 8 + r, :] = pre_sums[0:1, r * depth : (r + 1) * depth]

    def load_attention(block):
        return [load(grad_tokens.at[rows_of[block]], gs), load(n1_h.at[rows_of[block]], n1)]

    row_loads = load_attention(0)
    down, into, attn = (
        Scatter(place, g, o, flows_refs[i * per : (i + 1) * per])
        for i, (g, o) in enumerate(((g_down, out_down), (g_in, out_in), (g_attn, out_attn)))
    )
    order = down.order()
    inner = [i % ring.inner for i in range(1, ring.inner + 1)]

    def send_core(flow):
        for i in inner:
            for j in order:
                flow.to_core(i, j)

    def send_y(flow):
        for i in inner[:-1]:
            for j in order:
                flow.along_y(i, j)

    act_load.wait()

    def down_part(part):
        g_down[:, part] = rounded(dot(gsh[...], act[:, part], 0, 0))

    over_columns(hidden, down_part)
    send_core(down)
    qkvc_load = load(qkvc_h, qkvc)
    tok_load = load(tokens_h, tok)
    midh_load.wait()

    def in_part(part):
        g_in[:, part] = rounded(dot(midh[...], gpreh[:, part], 0, 0))

    over_columns(hidden, in_part)
    send_core(into)
    send_y(down)
    send_y(into)
    later = [functools.partial(down.along_z, j) for j in order]
    later += [functools.partial(into.along_z, j) for j in order]
    w1_load.wait()
    qkvc_load.wait()
    finals = []
    for block, rows in enumerate(rows_of):
        for copy in row_loads:
            copy.wait()
        received(backs[block])
        terms = [own[rows, :]] + [back_in[m, rows, :] for m in range(n_mp - 1)]
        normed = n1[...]
        grad_middle = gs[...] + spread(terms)
        grad = norm_back(grad_middle, normed, inv1[rows, 0:1], gains[0:1, :])
        gs[...] = grad
        gsumh[rows, :] = rounded(grad)
        if block + 1 < blocks:
            saving = load(gs, grad_tokens.at[rows])
        small[0:1, :] += column_sum(grad_middle * normed)
        small[1:2, :] += column_sum(grad_middle)
        small[2:3, :] += column_sum(grad)
        gctx[...] = rounded(dot(gsumh[rows, :], weights[:, 3 * width :]))
        if block + 1 < blocks:
            saving.wait()
            row_loads = load_attention(block + 1)
        if later:
            later.pop(0)()

        def pair_step(pair, carry, block=block):
            attend_back_pair(qkvc, seg_col, seg_row, lse, gctx, dqkv, small, block, pair)
            return carry

        lax.fori_loop(0, width // LANES, pair_step, 0)
        for copy in backs[block]:
            copy.wait_send()

        def to_input(part, rows=rows):
            own[rows, part] = rounded(dot(dqkv[rows, :], weights[part, : 3 * width], 1, 1))

        over_columns(depth, to_input)
        finals.append(cross.send(own.at[rows], lambda m: recv.at[m, rows], xs.at[block], xr.at[block]))
        if later:
            later.pop(0)()
    summing = Total(place, small, stages, inbox, (ts, tr)).steps()
    next(summing)
    tok_load.wait()

    def qkv_part(s, carry):
        part = pl.ds(pl.multiple_of(s * width, width), width)
        g_attn[:, part] = rounded(dot(tok[...], dqkv[:, part], 0, 0))
        return carry

    lax.fori_loop(0, 3, qkv_part, 0)
    g_attn[:, 3 * width :] = rounded(dot(gsumh[...], qkvc[:, 3 * width :], 0, 0))
    send_core(attn)
    for _ in summing:
        if later:
            later.pop(0)()
    out_small[...] = stages[2]
    send_y(attn)
    while later:
        later.pop(0)()
    for j in order:
        attn.along_z(j)
    for flow in (down, into, attn):
        flow.finish()

    def finish(block, total):
        rows = rows_of[block]
        received(finals[block])
        load(recv.at[:, rows], term_in).wait()
        total[...] += spread([own[rows, :]] + [term_in[m] for m in range(n_mp - 1)])
        return load(total, grad_tokens.at[rows])

    for block in range(blocks - 1):
        load(grad_tokens.at[rows_of[block]], n1).wait()
        finish(block, n1).wait()
    finish(blocks - 1, gs).wait()
    for copies in (*finals, crossing):
        for copy in copies:
            copy.wait_send()


def backward(ring, n_mp, gathered, kept, tokens, grad_output, lse, inv1, seg_col, seg_row, gains, biases):
    rows, depth = tokens.shape
    qkvc, act = kept[0], kept[1]
    width, hidden = qkvc.shape[1] // 4, act.shape[1]
    blocks = rows // BLOCK
    piece = depth // ring.n
    shape = jax.ShapeDtypeStruct
    small_rows = 8 * pl.cdiv(7 + hidden // depth, 8)
    peers = ring.core - 1 + ring.inner - 1 + ring.outer - 1
    half = lambda *dims: pltpu.VMEM(dims, HALF)
    full = lambda *dims: pltpu.VMEM(dims, FULL)
    flow = Scatter.scratch(ring, piece, hidden, HALF)
    return pl.pallas_call(
        functools.partial(backward_kernel, ring, n_mp),
        name="backward",
        out_shape=[shape((piece, hidden), FULL)] * 2
        + [shape((piece, 4 * width), FULL), shape((small_rows, depth), FULL), shape((rows, depth), HALF),
           shape((rows, depth), FULL), shape((rows, depth), HALF), shape((n_mp - 1, rows, depth), HALF)],
        in_specs=[ANY] * 12 + [VMEM] * 6,
        out_specs=[VMEM] * 4 + [ANY] * 2 + [VMEM, ANY],
        scratch_shapes=[
            half(depth, hidden), half(depth, hidden), half(depth, hidden), half(depth, hidden),
            half(rows, hidden), half(rows, depth), half(rows, depth), half(rows, 3 * width),
            full(BLOCK, depth), full(BLOCK, depth), half(BLOCK, depth),
            half(n_mp - 1, BLOCK, depth), half(n_mp - 1, BLOCK, depth), half(n_mp - 1, rows, depth),
            half(BLOCK, width), full(small_rows, depth), full(8, hidden),
            full(3, small_rows, depth), full(peers, small_rows, depth),
            DMA((16 + 12 * blocks,)), DMA((n_mp - 1,)), DMA((n_mp - 1,)),
            *[DMA((blocks, n_mp - 1))] * 4, DMA((peers,)), DMA((peers,)),
            *flow, *flow, *Scatter.scratch(ring, piece, 4 * width, HALF),
        ],
        compiler_params=pltpu.CompilerParams(
            collective_id=1, has_side_effects=True, vmem_limit_bytes=67043328
        ),
        cost_estimate=pl.CostEstimate(flops=int(4e10), bytes_accessed=int(2e8), transcendentals=0),
    )(*gathered, *kept, tokens, grad_output, lse, inv1, seg_col, seg_row, gains, biases)


def per_device(
    n_dp, n_mp,
    tokens, segments, grad_output, w_qkv, w_out, w_in, w_down, qv_bias, ffn_bias, gains, biases
):
    ring = Ring(n_dp)
    width, hidden = w_qkv.shape[2], w_in.shape[1]
    rows, depth = tokens.shape
    piece = depth // n_dp
    n_heads = width // HEAD

    shards = [jnp.concatenate([w_qkv[0], w_qkv[1], w_qkv[2], w_out.T], axis=1), w_in, w_down.T]
    seg_col = segments.reshape(rows, 1)
    seg_row = segments.reshape(-1, BLOCK)
    bias = qv_bias.reshape(2, width)
    bias = jnp.stack([bias[0], jnp.zeros_like(bias[0]), bias[1]])
    *kept, lse, inv1 = forward(
        ring, n_mp, tokens, seg_col, seg_row, bias, shards, ffn_bias.reshape(1, -1), gains, biases
    )
    grad_down, grad_in, grad_attn, small, output, grad_tokens, _, _ = backward(
        ring, n_mp, kept[:3], kept[3:], tokens, grad_output, lse, inv1, seg_col, seg_row, gains, biases
    )

    me = lax.axis_index("dp")
    bit = HEAD // n_dp
    norms = lax.dynamic_slice(small, (0, me * piece), (6, piece))
    heads = lax.dynamic_slice(small[6, : 2 * width].reshape(2, n_heads, HEAD), (0, 0, me * bit), (2, n_heads, bit))
    pre = small[7 : 7 + hidden // depth].reshape(-1, HEAD)
    return (
        output,
        grad_tokens,
        jnp.stack([grad_attn[:, s * width : (s + 1) * width] for s in range(3)]),
        grad_attn[:, 3 * width :].T,
        grad_in,
        grad_down.T,
        heads,
        lax.dynamic_slice(pre, (0, me * bit), (hidden // HEAD, bit)),
        jnp.stack([norms[0], norms[3]]),
        jnp.stack([norms[1], norms[4], norms[2], norms[5]]),
    )


def solution(mesh):
    n_dp, n_mp = mesh.shape["dp"], mesh.shape["mp"]
    placed = (
        P("dp", None),
        P("dp"),
        P("dp", None),
        P(None, "dp", "mp"),
        P("mp", "dp"),
        P("dp", "mp"),
        P("mp", "dp"),
        P(None, "mp", None),
        P("mp", None),
        P(),
        P(),
    )

    def body(*args):
        return per_device(n_dp, n_mp, *args)

    return jax.shard_map(
        body,
        mesh=mesh,
        in_specs=placed,
        out_specs=(
            P("dp", None),
            P("dp", None),
            P(None, "dp", "mp"),
            P("mp", "dp"),
            P("dp", "mp"),
            P("mp", "dp"),
            P(None, "mp", "dp"),
            P("mp", "dp"),
            P(None, "dp"),
            P(None, "dp"),
        ),
        check_vma=False,
    )
```

```python
import functools

import jax
import jax.numpy as jnp
from jax import lax
from jax.experimental import pallas as pl
from jax.experimental.pallas import tpu as pltpu
from jax.sharding import PartitionSpec as P

HEAD = 64
BLOCK = 512
CORES = 2
OUTER = 4
LANES = 128
CHUNK = 512

EPS = 1e-05
HALF = jnp.bfloat16
FULL = jnp.float32
MESH = pl.DeviceIdType.MESH
VMEM = pl.BlockSpec(memory_space=pltpu.VMEM)
ANY = pl.BlockSpec(memory_space=pl.ANY)
DMA = pltpu.SemaphoreType.DMA


def rounded(value):
    return value.astype(HALF)


def dot(left, right, left_dim=1, right_dim=0):
    return lax.dot_general(
        left, right, (((left_dim,), (right_dim,)), ((), ())), preferred_element_type=FULL
    )


def normalize(summed):
    centered = summed - jnp.mean(summed, axis=-1, keepdims=True)
    inv_std = lax.rsqrt(jnp.mean(centered * centered, axis=-1, keepdims=True) + EPS)
    return (centered * inv_std, inv_std)


def norm_back(grad_in, normed, inv_std, gain):
    scaled = grad_in * gain
    return inv_std * (
        scaled
        - jnp.mean(scaled, axis=-1, keepdims=True)
        - normed * jnp.mean(scaled * normed, axis=-1, keepdims=True)
    )


def column_sum(value):
    return jnp.sum(value, axis=0, keepdims=True)


class Ring:
    def __init__(self, n_dp):
        self.n = n_dp
        self.core = CORES
        self.outer = OUTER if n_dp % (OUTER * CORES) == 0 else 1
        self.inner = n_dp // (self.outer * self.core)

    def split(self, index):
        return index // (self.inner * self.core), (index // self.core) % self.inner, index % self.core

    def join(self, outer, inner, core):
        return (outer * self.inner + inner) * self.core + core


class Place:
    def __init__(self, ring):
        self.ring = ring
        self.z, self.y, self.c = ring.split(lax.axis_index("dp"))
        self.z_next = ring.join((self.z + 1) % ring.outer, self.y, self.c)
        self.z_last = ring.join((self.z + ring.outer - 1) % ring.outer, self.y, self.c)
        self.y_next = ring.join(self.z, (self.y + 1) % ring.inner, self.c)
        self.y_last = ring.join(self.z, (self.y + ring.inner - 1) % ring.inner, self.c)
        self.partner = ring.join(self.z, self.y, 1 - self.c)

    def at_z(self, k):
        return self.ring.join((self.z + k) % self.ring.outer, self.y, self.c)

    def at_y(self, k):
        return self.ring.join(self.z, (self.y + k) % self.ring.inner, self.c)

    def enter(self, n_mp=1):
        peers = [{"dp": self.partner}]
        peers += [{"dp": self.at_z(k)} for k in range(1, self.ring.outer)]
        peers += [{"dp": self.at_y(k)} for k in range(1, self.ring.inner)]
        x = lax.axis_index("mp")
        peers += [{"mp": (x + k) % n_mp} for k in range(1, n_mp)]
        barrier = pltpu.get_barrier_semaphore()
        for peer in peers:
            pl.semaphore_signal(barrier, inc=1, device_id=peer, device_id_type=MESH)
        pl.semaphore_wait(barrier, len(peers))


def copy_to(source, target, send_sem, recv_sem, device):
    return pltpu.make_async_remote_copy(
        src_ref=source, dst_ref=target, send_sem=send_sem, recv_sem=recv_sem,
        device_id=device, device_id_type=MESH,
    )


class Gather:
    def __init__(self, place, shard, out, sems):
        self.p, self.shard, self.out = place, shard, out
        self.own_sem, self.zs, self.zr, self.ys, self.yr, self.cs, self.cr = sems
        self.rows = shard.shape[0]
        self.sent, self.z_in, self.y_in, self.c_in = [], {}, {}, []
        self.own = pltpu.make_async_copy(shard, self.at(place.z, place.y, place.c), self.own_sem)

    def at(self, z, y, c):
        start = self.p.ring.join(z, y, c) * self.rows
        return self.out.at[pl.ds(pl.multiple_of(start, self.rows), self.rows)]

    def send(self, source, target, send_sem, recv_sem, device):
        copy = copy_to(source, target, send_sem, recv_sem, {"dp": device})
        copy.start()
        self.sent.append(copy)
        return copy

    def along_z(self, k):
        p, ring = self.p, self.p.ring
        target = self.at((p.z + ring.outer - k) % ring.outer, p.y, p.c)
        source = target
        if k == 0:
            self.own.start()
            source = self.shard
        else:
            self.z_in[k].wait_recv()
        if k < ring.outer - 1:
            self.z_in[k + 1] = self.send(source, target, self.zs.at[k], self.zr.at[k], p.z_next)
        if ring.inner > 1:
            self.y_in[k, 1] = self.send(source, target, self.ys.at[k, 0], self.yr.at[k, 0], p.y_next)
        self.c_in.append(self.send(source, target, self.cs.at[k, 0], self.cr.at[k, 0], p.partner))

    def along_y(self, k, step=1):
        p, ring = self.p, self.p.ring
        if step >= ring.inner:
            return
        target = self.at((p.z + ring.outer - k) % ring.outer, (p.y + ring.inner - step) % ring.inner, p.c)
        self.y_in[k, step].wait_recv()
        if step < ring.inner - 1:
            self.y_in[k, step + 1] = self.send(
                target, target, self.ys.at[k, step], self.yr.at[k, step], p.y_next
            )
        self.c_in.append(
            self.send(target, target, self.cs.at[k, step], self.cr.at[k, step], p.partner)
        )

    def rest_y(self, k):
        for step in range(2, self.p.ring.inner):
            self.along_y(k, step)

    def arrived(self):
        for copy in self.c_in:
            copy.wait_recv()
        self.own.wait()

    def finish(self):
        for copy in self.sent:
            copy.wait_send()

    @staticmethod
    def scratch(ring):
        z, y = max(ring.outer - 1, 1), max(ring.inner - 1, 1)
        return [
            DMA, DMA((z,)), DMA((z,)), DMA((ring.outer, y)), DMA((ring.outer, y)),
            DMA((ring.outer, ring.inner)), DMA((ring.outer, ring.inner)),
        ]


def attend_pair(qkvc, seg_col, seg_row, lse_ref, block, pair):
    width = qkvc.shape[1] // 4
    rows = pl.ds(block * BLOCK, BLOCK)

    def lanes(member):
        return pl.ds(pl.multiple_of(member * width + pair * LANES, LANES), LANES)

    queries = qkvc[rows, lanes(0)] * jnp.asarray(HEAD ** (-0.5), HALF)
    keys, values = qkvc[rows, lanes(1)], qkvc[rows, lanes(2)]
    lane = lax.broadcasted_iota(jnp.int32, (BLOCK, LANES), 1)
    same = seg_col[rows, :] == seg_row[pl.ds(block, 1), :]
    per_pair = LANES // HEAD
    context = jnp.zeros((BLOCK, LANES), FULL)
    log_totals = lse_ref[rows, :]
    for j in range(per_pair):
        mine = (lane // HEAD) == j
        score = jnp.where(same, dot(jnp.where(mine, queries, jnp.zeros_like(queries)), keys, 1, 1), -1e9)
        top = jnp.max(score, axis=1, keepdims=True)
        exps = jnp.exp(score - top)
        total = jnp.sum(exps, axis=1, keepdims=True)
        weights = rounded(exps * (1.0 / total))
        context = jnp.where(mine, dot(weights, values), context)
        log_totals = jnp.where(lane == per_pair * pair + j, top + jnp.log(total), log_totals)
    lse_ref[rows, :] = log_totals
    qkvc[rows, lanes(3)] = rounded(context)


def over_columns(columns, body):
    chunk = min(CHUNK, columns)

    def step(j, carry):
        body(pl.ds(pl.multiple_of(j * chunk, chunk), chunk))
        return carry

    lax.fori_loop(0, columns // chunk, step, 0)


def spread(terms):
    total = terms[0].astype(FULL)
    for term in terms[1:]:
        total = total + term.astype(FULL)
    return total


class Cross:
    def __init__(self, n_mp):
        self.n_mp, self.x = n_mp, lax.axis_index("mp")

    def send(self, source, target, send_sems, recv_sems):
        copies = []
        for m in range(1, self.n_mp):
            copy = copy_to(
                source, target(m - 1), send_sems.at[m - 1], recv_sems.at[m - 1],
                {"mp": (self.x + m) % self.n_mp},
            )
            copy.start()
            copies.append(copy)
        return copies


def received(copies):
    for copy in copies:
        copy.wait_recv()


def forward_kernel(ring, n_mp, *refs):
    tok, seg_col, seg_row, bias, s1, s2, s3, hidden_bias, gains, biases = refs[:10]
    g1, g2, g3, qkvc_out, act_out, slope_out, midh_out, n1_out, own_out, recv_out, lse, inv1 = refs[10:22]
    w1, w2, w3, qkvc, own, recv, act, slope, midh, n1, term, term_in = refs[22:34]
    stores, xs, xr, fs, fr = refs[34:39]
    sems = refs[39:]
    per = len(sems) // 3
    place = Place(ring)
    place.enter(n_mp)
    cross = Cross(n_mp)
    first, second, third = (
        Gather(place, s, g, sems[i * per : (i + 1) * per])
        for i, (s, g) in enumerate(((s1, w1), (s2, w2), (s3, w3)))
    )
    width = qkvc.shape[1] // 4
    depth, hidden = tok.shape[1], act.shape[1]
    blocks = tok.shape[0] // BLOCK
    saving = []

    def save(source, target):
        copy = pltpu.make_async_copy(source, target, stores.at[len(saving)])
        copy.start()
        saving.append(copy)

    last = ring.outer
    for k in range(last):
        first.along_z(k)
        if k >= 1:
            first.along_y(k - 1)
    second.along_z(0)
    first.along_y(last - 1)
    for k in range(last):
        first.rest_y(k)
    z2 = [functools.partial(second.along_z, k) for k in range(1, last)]
    z3 = [functools.partial(third.along_z, k) for k in range(last)]
    first.arrived()
    lse[...] = jnp.zeros_like(lse)

    def relay(steps):
        if steps:
            steps.pop(0)()

    relay(z2)
    crossing, attended, ffn_terms = [], [], []
    for block in range(blocks):
        rows = pl.ds(block * BLOCK, BLOCK)

        def project(s, carry, rows=rows):
            part = pl.ds(pl.multiple_of(s * width, width), width)
            qkvc[rows, part] = rounded(dot(tok[rows, :], w1[:, part]) + bias[pl.ds(s, 1), :])
            return carry

        lax.fori_loop(0, 3, project, 0)

        def pair_step(pair, carry, block=block):
            attend_pair(qkvc, seg_col, seg_row, lse, block, pair)
            return carry

        lax.fori_loop(0, width // LANES, pair_step, 0)
        own[rows, :] = rounded(dot(qkvc[rows, 3 * width :], w1[:, 3 * width :], 1, 1))
        attended.append(cross.send(own.at[rows], lambda m: recv.at[m, rows], xs.at[block], xr.at[block]))
        relay(z2)
        relay(z3)
    save(w1, g1)
    save(qkvc, qkvc_out)
    while z2:
        relay(z2)
    for k in range(last):
        relay(z3)
        second.along_y(k)
        second.rest_y(k)
    while z3:
        relay(z3)
    second.arrived()
    save(w2, g2)
    for block in range(blocks):
        rows = pl.ds(block * BLOCK, BLOCK)
        received(attended[block])
        crossing += attended[block]
        terms = [own[rows, :]] + [recv[m, rows, :] for m in range(n_mp - 1)]
        summed = tok[rows, :].astype(FULL) + spread(terms) + biases[2:3, :]
        normed, inv = normalize(summed)
        n1[rows, :] = normed
        inv1[rows, :] = jnp.broadcast_to(inv, (BLOCK, LANES))
        midh[rows, :] = rounded(normed * gains[0:1, :] + biases[0:1, :])

        def up(part, rows=rows):
            pre = dot(midh[rows, :], w2[:, part]) + hidden_bias[:, part]
            phi = 0.5 * (1.0 + lax.erf(pre * 0.7071067811865476))
            act[rows, part] = rounded(pre * phi)
            slope[rows, part] = rounded(phi + pre * jnp.exp(-0.5 * pre * pre) * 0.3989422804014327)

        over_columns(hidden, up)
        if block == 0:
            for k in range(last):
                third.along_y(k)
                third.rest_y(k)
            third.arrived()
            save(w3, g3)

        def down(part, rows=rows):
            term[rows, part] = rounded(dot(act[rows, :], w3[part, :], 1, 1))

        over_columns(depth, down)
        if block + 1 < blocks:
            ffn_terms.append(
                cross.send(term.at[rows], lambda m: term_in.at[m, rows], fs.at[block], fr.at[block])
            )
    save(act, act_out)
    save(slope, slope_out)
    save(midh, midh_out)
    save(n1, n1_out)
    save(term, own_out)
    for copies in ffn_terms:
        received(copies)
        crossing += copies
    save(term_in, recv_out)
    for gather in (first, second, third):
        gather.finish()
    for copy in crossing:
        copy.wait_send()
    for copy in saving:
        copy.wait()


def forward(ring, n_mp, tokens, seg_col, seg_row, bias, shards, hidden_bias, gains, biases):
    rows, depth = tokens.shape
    width, hidden = bias.shape[1], hidden_bias.shape[1]
    blocks = rows // BLOCK
    shape = jax.ShapeDtypeStruct
    gathered = [(ring.n * s.shape[0], s.shape[1]) for s in shards]
    early = (blocks - 1) * BLOCK
    kept = [
        *((dims, HALF) for dims in gathered), ((rows, 4 * width), HALF), ((rows, hidden), HALF),
        ((rows, hidden), HALF), ((rows, depth), HALF), ((rows, depth), FULL), ((rows, depth), HALF),
        ((n_mp - 1, early, depth), HALF),
    ]
    scratch = [pltpu.VMEM(dims, kind) for dims, kind in kept]
    partial = [pltpu.VMEM((rows, depth), HALF), pltpu.VMEM((n_mp - 1, rows, depth), HALF)]
    return pl.pallas_call(
        functools.partial(forward_kernel, ring, n_mp),
        name="forward",
        out_shape=[shape(dims, kind) for dims, kind in kept] + [shape((rows, LANES), FULL)] * 2,
        in_specs=[VMEM] * 10,
        out_specs=[ANY] * len(kept) + [VMEM] * 2,
        scratch_shapes=scratch[:4] + partial + scratch[4:]
        + [DMA((len(kept),))] + [DMA((blocks, n_mp - 1))] * 4 + Gather.scratch(ring) * 3,
        compiler_params=pltpu.CompilerParams(
            collective_id=0, has_side_effects=True, vmem_limit_bytes=60 << 20
        ),
        cost_estimate=pl.CostEstimate(flops=int(2e10), bytes_accessed=int(2e8), transcendentals=0),
    )(tokens, seg_col, seg_row, bias, *shards, hidden_bias, gains, biases)


class Scatter:
    def __init__(self, place, grad, out, bufs):
        self.p, self.grad, self.out = place, grad, out
        self.rows = out.shape[0]
        (self.c_in, self.y_in, self.z_in, self.cs, self.cr, self.ys, self.yr, self.zs, self.zr) = bufs
        self.sent, self.c_copy, self.y_copy, self.z_copy = [], {}, {}, {}

    def block(self, z, y, c):
        start = self.p.ring.join(z, y, c) * self.rows
        return self.grad.at[pl.ds(pl.multiple_of(start, self.rows), self.rows)]

    def z_of(self, j):
        return (self.p.z + self.p.ring.outer - j) % self.p.ring.outer

    def y_of(self, i):
        return (self.p.y + self.p.ring.inner - i) % self.p.ring.inner

    def send(self, source, target, send_sem, recv_sem, device):
        copy = copy_to(source, target, send_sem, recv_sem, {"dp": device})
        copy.start()
        self.sent.append(copy)
        return copy

    def order(self):
        outer = self.p.ring.outer
        return [j % outer for j in range(1, outer + 1)]

    def to_core(self, i, j):
        p = self.p
        self.c_copy[i, j] = self.send(
            self.block(self.z_of(j), self.y_of(i), 1 - p.c), self.c_in.at[i, j],
            self.cs.at[i, j], self.cr.at[i, j], p.partner,
        )

    def chip_sum(self, i, j):
        self.c_copy[i, j].wait_recv()
        return self.block(self.z_of(j), self.y_of(i), self.p.c)[...].astype(FULL) + self.c_in[i, j].astype(FULL)

    def along_y(self, i, j):
        total = self.chip_sum(i, j)
        if i > 1:
            self.y_copy[i - 1, j].wait_recv()
            total = total + self.y_in[i - 2, j].astype(FULL)
        self.c_in[i, j] = total.astype(self.c_in.dtype)
        self.y_copy[i, j] = self.send(
            self.c_in.at[i, j], self.y_in.at[i - 1, j],
            self.ys.at[i - 1, j], self.yr.at[i - 1, j], self.p.y_next,
        )

    def along_z(self, j):
        ring = self.p.ring
        total = self.chip_sum(0, j)
        if ring.inner > 1:
            self.y_copy[ring.inner - 1, j].wait_recv()
            total = total + self.y_in[ring.inner - 2, j].astype(FULL)
        step = j if j else ring.outer
        if step > 1:
            self.z_copy[step - 1].wait_recv()
            total = total + self.z_in[step - 2].astype(FULL)
        if j == 0:
            self.out[...] = total
        else:
            self.c_in[0, j] = total.astype(self.c_in.dtype)
            self.z_copy[j] = self.send(
                self.c_in.at[0, j], self.z_in.at[j - 1], self.zs.at[j - 1], self.zr.at[j - 1],
                self.p.z_next,
            )

    def finish(self):
        for copy in self.sent:
            copy.wait_send()

    @staticmethod
    def scratch(ring, rows, columns, dtype):
        z, y = max(ring.outer - 1, 1), max(ring.inner - 1, 1)

        def buf(*lead):
            return pltpu.VMEM((*lead, rows, columns), dtype)

        return [
            buf(ring.inner, ring.outer), buf(y, ring.outer), buf(z),
            DMA((ring.inner, ring.outer)), DMA((ring.inner, ring.outer)),
            DMA((y, ring.outer)), DMA((y, ring.outer)), DMA((z,)), DMA((z,)),
        ]


def attend_back_pair(qkvc, seg_col, seg_row, lse, gctx, dqkv, small, block, pair):
    rows = pl.ds(block * BLOCK, BLOCK)
    width = qkvc.shape[1] // 4

    def lanes(member):
        return pl.ds(pl.multiple_of(member * width + pair * LANES, LANES), LANES)

    q, keys, values = qkvc[rows, lanes(0)], qkvc[rows, lanes(1)], qkvc[rows, lanes(2)]
    queries = q * jnp.asarray(HEAD ** (-0.5), HALF)
    grad = gctx[:, lanes(0)]
    product = grad.astype(FULL) * qkvc[rows, lanes(3)].astype(FULL)
    lane = lax.broadcasted_iota(jnp.int32, (BLOCK, LANES), 1)
    same = seg_col[rows, :] == seg_row[pl.ds(block, 1), :]
    per_pair = LANES // HEAD
    log_totals = lse[rows, :]
    grad_q = grad_k = grad_v = jnp.zeros((BLOCK, LANES), FULL)
    for j in range(per_pair):
        mine = (lane // HEAD) == j
        zero = jnp.zeros_like(grad)
        score = jnp.where(same, dot(jnp.where(mine, queries, zero), keys, 1, 1), -1e9)
        log_total = jnp.sum(jnp.where(lane == per_pair * pair + j, log_totals, 0.0), axis=1, keepdims=True)
        delta = jnp.sum(jnp.where(mine, product, 0.0), axis=1, keepdims=True)
        prob = jnp.exp(score - log_total)
        grad_prob = dot(jnp.where(mine, grad, zero), values, 1, 1)
        grad_score = rounded(prob * (grad_prob - delta) * HEAD ** (-0.5))
        grad_q = jnp.where(mine, dot(grad_score, keys), grad_q)
        grad_k = jnp.where(mine, dot(grad_score, q, 0, 0), grad_k)
        grad_v = jnp.where(mine, dot(rounded(prob), grad, 0, 0), grad_v)
    for member, part in enumerate((grad_q, grad_k, grad_v)):
        dqkv[rows, lanes(member)] = rounded(part)
    small[6:7, lanes(0)] += column_sum(grad_q)
    small[6:7, lanes(1)] += column_sum(grad_v)


class Total:
    def __init__(self, place, value, stages, inbox, sems):
        self.p, self.value, self.stages, self.inbox = place, value, stages, inbox
        self.ss, self.rs = sems
        self.sent = []

    def stage(self, number, devices, first):
        source = self.value if number == 0 else self.stages.at[number - 1]
        copies = []
        for k, device in enumerate(devices):
            slot = first + k
            copy = copy_to(source, self.inbox.at[slot], self.ss.at[slot], self.rs.at[slot], {"dp": device})
            copy.start()
            copies.append(copy)
        self.sent += copies
        return copies

    def steps(self):
        ring = self.p.ring
        groups = [
            [self.p.partner],
            [self.p.at_y(k) for k in range(1, ring.inner)],
            [self.p.at_z(k) for k in range(1, ring.outer)],
        ]
        first = 0
        for number, devices in enumerate(groups):
            copies = self.stage(number, devices, first)
            yield
            total = (self.value if number == 0 else self.stages.at[number - 1])[...]
            for k, copy in enumerate(copies):
                copy.wait_recv()
                total = total + self.inbox[first + k]
            self.stages[number] = total
            first += len(devices)
        for copy in self.sent:
            copy.wait_send()


def backward_kernel(ring, n_mp, *refs):
    (w1_h, w2_h, w3_h, qkvc_h, act_h, slope_h, midh_h, n1_h, term_h, recv_h, tokens_h, up_h,
     lse, inv1, seg_col, seg_row, gains, biases) = refs[:18]
    out_down, out_in, out_attn, out_small, output, grad_tokens, own, recv = refs[18:26]
    (weights, g_down, g_in, g_attn, qkvc, tok, gsumh, dqkv, n1, gs, up, term_in, last_in, back_in,
     gctx, small, pre_sums, stages, inbox) = refs[26:45]
    loads, ls, lr, bs, br, xs, xr, ts, tr = refs[45:54]
    flows_refs = refs[54:]
    per = len(flows_refs) // 3
    act, gsh, midh, gpreh = qkvc, tok, gsumh, g_attn
    place = Place(ring)
    place.enter(n_mp)
    cross = Cross(n_mp)
    rows_all, depth = own.shape
    width, hidden = qkvc.shape[1] // 4, g_attn.shape[1]
    blocks = rows_all // BLOCK
    rows_of = [pl.ds(block * BLOCK, BLOCK) for block in range(blocks)]
    used = []

    def load(source, target):
        copy = pltpu.make_async_copy(source, target, loads.at[len(used)])
        used.append(copy)
        copy.start()
        return copy

    def load_rows(block):
        rows = rows_of[block]
        copies = [load(n1_h.at[rows], n1), load(up_h.at[rows], up), load(term_h.at[rows], own.at[rows])]
        if block + 1 < blocks:
            copies.append(load(recv_h.at[:, rows], term_in))
        return copies

    last = rows_of[-1]
    last_copies = cross.send(term_h.at[last], lambda m: last_in.at[m], ls, lr)
    row_loads = load_rows(0)
    w3_load = load(w3_h, weights)
    slope_load = load(slope_h, gpreh)
    w2_load = load(w2_h, g_in)
    act_load = load(act_h, act)
    midh_load = load(midh_h, midh)
    small[...] = jnp.zeros_like(small)
    pre_sums[...] = jnp.zeros_like(pre_sums)
    crossing, backs = list(last_copies), []
    for block, rows in enumerate(rows_of):
        for copy in row_loads:
            copy.wait()
        if block == blocks - 1:
            received(last_copies)
            others = [last_in[m] for m in range(n_mp - 1)]
        else:
            others = [term_in[m] for m in range(n_mp - 1)]
        middle = n1[...] * gains[0:1, :] + biases[0:1, :]
        second = middle + spread([own[rows, :]] + others) + biases[3:4, :]
        normed, inv = normalize(second)
        upstream = up[...].astype(FULL)
        grad = norm_back(upstream, normed, inv, gains[1:2, :])
        small[3:4, :] += column_sum(upstream * normed)
        small[4:5, :] += column_sum(upstream)
        small[5:6, :] += column_sum(grad)
        up[...] = rounded(normed * gains[1:2, :] + biases[1:2, :])
        gs[...] = grad
        gsh[rows, :] = rounded(grad)
        saving = [load(up, output.at[rows]), load(gs, grad_tokens.at[rows])]
        if block == 0:
            w3_load.wait()
            slope_load.wait()

        def to_hidden(part, rows=rows):
            grad_pre = dot(gsh[rows, :], weights[:, part]) * gpreh[rows, part].astype(FULL)
            pre_sums[0:1, part] += column_sum(grad_pre)
            gpreh[rows, part] = rounded(grad_pre)

        over_columns(hidden, to_hidden)
        for copy in saving:
            copy.wait()
        if block + 1 < blocks:
            row_loads = load_rows(block + 1)
        else:
            w1_load = load(w1_h, weights)
        if block == 0:
            w2_load.wait()

        def to_model(part, rows=rows):
            own[rows, part] = rounded(dot(gpreh[rows, :], g_in[part, :], 1, 1))

        over_columns(depth, to_model)
        backs.append(cross.send(own.at[rows], lambda m: back_in.at[m, rows], bs.at[block], br.at[block]))
    for r in range(hidden // depth):
        small[7 + r : 8 + r, :] = pre_sums[0:1, r * depth : (r + 1) * depth]

    def load_attention(block):
        return [load(grad_tokens.at[rows_of[block]], gs), load(n1_h.at[rows_of[block]], n1)]

    row_loads = load_attention(0)
    down, into, attn = (
        Scatter(place, g, o, flows_refs[i * per : (i + 1) * per])
        for i, (g, o) in enumerate(((g_down, out_down), (g_in, out_in), (g_attn, out_attn)))
    )
    order = down.order()
    inner = [i % ring.inner for i in range(1, ring.inner + 1)]

    def send_core(flow):
        for i in inner:
            for j in order:
                flow.to_core(i, j)

    def send_y(flow):
        for i in inner[:-1]:
            for j in order:
                flow.along_y(i, j)

    act_load.wait()

    def down_part(part):
        g_down[:, part] = rounded(dot(gsh[...], act[:, part], 0, 0))

    over_columns(hidden, down_part)
    send_core(down)
    qkvc_load = load(qkvc_h, qkvc)
    tok_load = load(tokens_h, tok)
    midh_load.wait()

    def in_part(part):
        g_in[:, part] = rounded(dot(midh[...], gpreh[:, part], 0, 0))

    over_columns(hidden, in_part)
    send_core(into)
    send_y(down)
    send_y(into)
    later = [functools.partial(down.along_z, j) for j in order]
    later += [functools.partial(into.along_z, j) for j in order]

    def relay(count=1):
        for _ in range(min(count, len(later))):
            later.pop(0)()

    w1_load.wait()
    qkvc_load.wait()
    finals = []
    for block, rows in enumerate(rows_of):
        for copy in row_loads:
            copy.wait()
        if block:
            relay()
        received(backs[block])
        terms = [own[rows, :]] + [back_in[m, rows, :] for m in range(n_mp - 1)]
        normed = n1[...]
        grad_middle = gs[...] + spread(terms)
        grad = norm_back(grad_middle, normed, inv1[rows, 0:1], gains[0:1, :])
        gs[...] = grad
        gsumh[rows, :] = rounded(grad)
        if block + 1 < blocks:
            saving = load(gs, grad_tokens.at[rows])
        small[0:1, :] += column_sum(grad_middle * normed)
        small[1:2, :] += column_sum(grad_middle)
        small[2:3, :] += column_sum(grad)
        gctx[...] = rounded(dot(gsumh[rows, :], weights[:, 3 * width :]))
        if block + 1 < blocks:
            saving.wait()
            row_loads = load_attention(block + 1)
        if block == 0:
            relay()

        def pair_step(pair, carry, block=block):
            attend_back_pair(qkvc, seg_col, seg_row, lse, gctx, dqkv, small, block, pair)
            return carry

        lax.fori_loop(0, width // LANES, pair_step, 0)
        for copy in backs[block]:
            copy.wait_send()

        def to_input(part, rows=rows):
            own[rows, part] = rounded(dot(dqkv[rows, :], weights[part, : 3 * width], 1, 1))

        over_columns(depth, to_input)
        finals.append(cross.send(own.at[rows], lambda m: recv.at[m, rows], xs.at[block], xr.at[block]))
        relay(2 if block else 1)
    summing = Total(place, small, stages, inbox, (ts, tr)).steps()
    next(summing)
    tok_load.wait()

    def qkv_part(s, carry):
        part = pl.ds(pl.multiple_of(s * width, width), width)
        g_attn[:, part] = rounded(dot(tok[...], dqkv[:, part], 0, 0))
        return carry

    lax.fori_loop(0, 3, qkv_part, 0)
    g_attn[:, 3 * width :] = rounded(dot(gsumh[...], qkvc[:, 3 * width :], 0, 0))
    send_core(attn)
    next(summing)
    relay()
    send_y(attn)

    def finish(block, total):
        rows = rows_of[block]
        received(finals[block])
        load(recv.at[:, rows], term_in).wait()
        total[...] += spread([own[rows, :]] + [term_in[m] for m in range(n_mp - 1)])
        return load(total, grad_tokens.at[rows])

    relay()
    attn.along_z(order[0])
    relay(len(later))
    next(summing)
    for block in range(blocks - 1):
        load(grad_tokens.at[rows_of[block]], n1).wait()
        finish(block, n1).wait()
    for j in order[1:-1]:
        attn.along_z(j)
    saving = finish(blocks - 1, gs)
    for j in order[1:][-1:]:
        attn.along_z(j)
    for _ in summing:
        pass
    out_small[...] = stages[2]
    for flow in (down, into, attn):
        flow.finish()
    saving.wait()
    for copies in (*finals, crossing):
        for copy in copies:
            copy.wait_send()


def backward(ring, n_mp, gathered, kept, tokens, grad_output, lse, inv1, seg_col, seg_row, gains, biases):
    rows, depth = tokens.shape
    qkvc, act = kept[0], kept[1]
    width, hidden = qkvc.shape[1] // 4, act.shape[1]
    blocks = rows // BLOCK
    piece = depth // ring.n
    shape = jax.ShapeDtypeStruct
    small_rows = 8 * pl.cdiv(7 + hidden // depth, 8)
    peers = ring.core - 1 + ring.inner - 1 + ring.outer - 1
    half = lambda *dims: pltpu.VMEM(dims, HALF)
    full = lambda *dims: pltpu.VMEM(dims, FULL)
    flow = Scatter.scratch(ring, piece, hidden, HALF)
    return pl.pallas_call(
        functools.partial(backward_kernel, ring, n_mp),
        name="backward",
        out_shape=[shape((piece, hidden), FULL)] * 2
        + [shape((piece, 4 * width), FULL), shape((small_rows, depth), FULL), shape((rows, depth), HALF),
           shape((rows, depth), FULL), shape((rows, depth), HALF), shape((n_mp - 1, rows, depth), HALF)],
        in_specs=[ANY] * 12 + [VMEM] * 6,
        out_specs=[VMEM] * 4 + [ANY] * 2 + [VMEM, ANY],
        scratch_shapes=[
            half(depth, hidden), half(depth, hidden), half(depth, hidden), half(depth, hidden),
            half(rows, hidden), half(rows, depth), half(rows, depth), half(rows, 3 * width),
            full(BLOCK, depth), full(BLOCK, depth), half(BLOCK, depth),
            half(n_mp - 1, BLOCK, depth), half(n_mp - 1, BLOCK, depth), half(n_mp - 1, rows, depth),
            half(BLOCK, width), full(small_rows, depth), full(8, hidden),
            full(3, small_rows, depth), full(peers, small_rows, depth),
            DMA((16 + 12 * blocks,)), DMA((n_mp - 1,)), DMA((n_mp - 1,)),
            *[DMA((blocks, n_mp - 1))] * 4, DMA((peers,)), DMA((peers,)),
            *flow, *flow, *Scatter.scratch(ring, piece, 4 * width, HALF),
        ],
        compiler_params=pltpu.CompilerParams(
            collective_id=1, has_side_effects=True, vmem_limit_bytes=67043328
        ),
        cost_estimate=pl.CostEstimate(flops=int(4e10), bytes_accessed=int(2e8), transcendentals=0),
    )(*gathered, *kept, tokens, grad_output, lse, inv1, seg_col, seg_row, gains, biases)


def per_device(
    n_dp, n_mp,
    tokens, segments, grad_output, w_qkv, w_out, w_in, w_down, qv_bias, ffn_bias, gains, biases
):
    ring = Ring(n_dp)
    width, hidden = w_qkv.shape[2], w_in.shape[1]
    rows, depth = tokens.shape
    piece = depth // n_dp
    n_heads = width // HEAD

    shards = [jnp.concatenate([w_qkv[0], w_qkv[1], w_qkv[2], w_out.T], axis=1), w_in, w_down.T]
    seg_col = segments.reshape(rows, 1)
    seg_row = segments.reshape(-1, BLOCK)
    bias = qv_bias.reshape(2, width)
    bias = jnp.stack([bias[0], jnp.zeros_like(bias[0]), bias[1]])
    *kept, lse, inv1 = forward(
        ring, n_mp, tokens, seg_col, seg_row, bias, shards, ffn_bias.reshape(1, -1), gains, biases
    )
    grad_down, grad_in, grad_attn, small, output, grad_tokens, _, _ = backward(
        ring, n_mp, kept[:3], kept[3:], tokens, grad_output, lse, inv1, seg_col, seg_row, gains, biases
    )

    me = lax.axis_index("dp")
    bit = HEAD // n_dp
    norms = lax.dynamic_slice(small, (0, me * piece), (6, piece))
    heads = lax.dynamic_slice(small[6, : 2 * width].reshape(2, n_heads, HEAD), (0, 0, me * bit), (2, n_heads, bit))
    pre = small[7 : 7 + hidden // depth].reshape(-1, HEAD)
    return (
        output,
        grad_tokens,
        jnp.stack([grad_attn[:, s * width : (s + 1) * width] for s in range(3)]),
        grad_attn[:, 3 * width :].T,
        grad_in,
        grad_down.T,
        heads,
        lax.dynamic_slice(pre, (0, me * bit), (hidden // HEAD, bit)),
        jnp.stack([norms[0], norms[3]]),
        jnp.stack([norms[1], norms[4], norms[2], norms[5]]),
    )


def solution(mesh):
    n_dp, n_mp = mesh.shape["dp"], mesh.shape["mp"]
    placed = (
        P("dp", None),
        P("dp"),
        P("dp", None),
        P(None, "dp", "mp"),
        P("mp", "dp"),
        P("dp", "mp"),
        P("mp", "dp"),
        P(None, "mp", None),
        P("mp", None),
        P(),
        P(),
    )

    def body(*args):
        return per_device(n_dp, n_mp, *args)

    return jax.shard_map(
        body,
        mesh=mesh,
        in_specs=placed,
        out_specs=(
            P("dp", None),
            P("dp", None),
            P(None, "dp", "mp"),
            P("mp", "dp"),
            P("dp", "mp"),
            P("mp", "dp"),
            P(None, "mp", "dp"),
            P("mp", "dp"),
            P(None, "dp"),
            P(None, "dp"),
        ),
        check_vma=False,
    )
```
